32 devices in a mesh: dp: 4 (over x, core), tensor: 8 (over z, y).
Axes of the slice: x: 2, y: 2, z: 4, core: 2. Of those that a mesh axis runs over, the one named last changes fastest.
Arguments:
- activations: bfloat16 [768, 4608], P(('dp', 'tensor')), may hold values from -0.43164062 to 0.43164062
- grad_out: bfloat16 [768, 18432], P('dp', 'tensor'), may hold values from -3 to 3
- weight: bfloat16 [4608, 18432], P(None, 'tensor'), may hold values from -0.09375 to 0.09375
Outputs:
- input_grad: bfloat16 [768, 4608], P(('dp', 'tensor'))
- weight_grad: float32 [4608, 18432], P('dp', 'tensor')
The draws below stay inside these ranges and needn't reach their ends.
All inputs are finite; a program needn't handle non-finite values.
Results may differ from the reference program's by a relative error of at most 0.001.
Values may be sent and summed in bfloat16 or wider, within the bound.
No kernel may reach another device: no remote copies, remote signals or barrier semaphores. Data moves between devices by JAX's collectives and lax.ppermute only.
A program may use at most 128 MiB of HBM per device.

```python
import jax
import jax.numpy as jnp

D = 4608
FF = 18432
REPLICA_TOK = 192
TOKENS = 768
N_DP = 4


def with_spikes(result, stream_key, source, target, shards_of, factor):
    def block_of(dim):
        return (jnp.arange(result.shape[dim]) // (result.shape[dim] // shards_of)).reshape((-1,) + (1,) * (result.ndim - 1 - dim))

    near = jax.random.permutation(stream_key, shards_of)[block_of(target)]
    other_side = (block_of(target) + shards_of // 2) % shards_of
    return jnp.where((block_of(source) == near) | (block_of(source) == other_side), factor * result, result)


def steps_of(key, shape, pieces, smallest, largest):
    factor_of, own = 1.0, jax.random.fold_in(key, 6)
    for dim, shards_of in pieces:
        draws = jnp.exp(jax.random.uniform(jax.random.fold_in(own, dim), (shards_of,), jnp.float32, smallest / len(pieces), largest / len(pieces)))
        factor_of = factor_of * jnp.repeat(draws, shape[dim] // shards_of).reshape([-1 if axis == dim else 1 for axis in range(len(shape))])
    return factor_of


def bell_draw(own_key, dims, spread, limit, split=(), kind=jnp.bfloat16):
    drawn = spread * jax.random.normal(own_key, dims, jnp.float32)
    if split:
        drawn = drawn * steps_of(own_key, dims, split, -0.22, 0.18)
    return jnp.clip(drawn, -limit, limit).astype(kind)


def heavy_noise(key, extent, spread, most, split, heavy, kind=jnp.bfloat16):
    values = spread * jax.random.normal(key, extent, jnp.float32)
    if split:
        values = values * steps_of(key, extent, split, -0.22, 0.18)
    return jnp.clip(with_spikes(values, jax.random.fold_in(key, 3), *heavy), -most, most).astype(kind)


def setup_inputs(seed: int = 0) -> dict:
    arg_keys = jax.random.split(jax.random.key(seed), 4)
    activations = heavy_noise(arg_keys[0], (TOKENS, D), (2 * (REPLICA_TOK * N_DP) ** -0.5), 0.43164062, ((0, 32),), (0, 1, 32, 2.75))
    grad_out = heavy_noise(arg_keys[1], (TOKENS, FF), 0.5, 3.0, ((0, 4), (1, 8)), (1, 0, 8, 2.0))
    weight = bell_draw(arg_keys[2], (D, FF), D ** -0.5, 0.09375, ((1, 8),))
    return {"activations": activations, "grad_out": grad_out, "weight": weight}


def reference(activations, grad_out, weight):
    input_grad = jnp.dot(grad_out, weight.T, preferred_element_type=jnp.float32).astype(jnp.bfloat16)
    weight_grad = jnp.dot(activations.T, grad_out, preferred_element_type=jnp.float32)
    return input_grad, weight_grad
```

```python
import jax
import jax.numpy as jnp
from jax import lax
from jax.sharding import PartitionSpec as P


def flip(value, axis, bit):
    pairs = [(i, i ^ bit) for i in range(lax.axis_size(axis))]
    return lax.ppermute(value, axis, pairs)


def shift(value, axis, step):
    size = lax.axis_size(axis)
    return lax.ppermute(value, axis, [(i, (i + step) % size) for i in range(size)])


def bits_of(size):
    bits = [1 << k for k in range(size.bit_length() - 1)]
    assert 1 << len(bits) == size
    return bits


def halves(blocks, mine):
    kept = lax.dynamic_index_in_dim(blocks, mine, 1, keepdims=False)
    sent = lax.dynamic_index_in_dim(blocks, 1 - mine, 1, keepdims=False)
    return kept, sent


def scatter_sum(partial, axis):
    size = lax.axis_size(axis)
    me = lax.axis_index(axis)
    rows, cols = partial.shape
    running = partial.reshape(size, rows // size, cols)
    for bit in bits_of(size):
        pairs = running.reshape(running.shape[0] // 2, 2, rows // size, cols)
        kept, sent = halves(pairs, (me // bit) % 2)
        running = kept + flip(sent, axis, bit)
    return running[0]


def gather_blocks(block, axis):
    size = lax.axis_size(axis)
    me = lax.axis_index(axis)
    held = block[None]
    for bit in reversed(bits_of(size)):
        other = flip(held, axis, bit)
        mine = (me // bit) % 2
        low = jnp.where(mine == 0, held, other)
        high = jnp.where(mine == 0, other, held)
        held = jnp.stack([low, high], 1).reshape(2 * held.shape[0], *held.shape[1:])
    return held


def on_device(activations, grad_out, weight):
    replicas = lax.axis_size("dp")
    ranks = lax.axis_size("tensor")
    chips = replicas // 2
    me = lax.axis_index("dp")
    chip, core = me // 2, me % 2
    shard_rows, features = activations.shape
    wide = features // chips

    def block_for(step):
        return lax.dynamic_slice_in_dim(activations, ((chip + step) % chips) * wide, wide, 1)

    rows = [block_for(0)] + [shift(block_for(k), "dp", 2 * k) for k in range(1, chips)]
    grads_near = flip(grad_out, "dp", 1)
    grads_far = [shift(grad_out, "dp", 2 * k) for k in range(1, chips)]
    partial = lax.dot_general(
        grad_out, weight, (((1,), (1,)), ((), ())), preferred_element_type=jnp.float32
    )
    held = gather_blocks(jnp.stack(rows), "tensor")
    held = held.transpose(1, 0, 2, 3).reshape(chips * ranks * shard_rows, 2, wide // 2)
    kept, sent = halves(held, core)
    columns = jnp.concatenate([kept, flip(sent, "dp", 1)])
    grads = jnp.concatenate(
        [grad_out, *grads_far, grads_near, *[flip(g, "dp", 1) for g in grads_far]]
    )
    input_grad = scatter_sum(partial, "tensor").astype(jnp.bfloat16)
    weight_grad = lax.dot_general(
        columns, grads, (((0,), (0,)), ((), ())), preferred_element_type=jnp.float32
    )
    return (input_grad, weight_grad)


def solution(mesh):
    placed = (P(("dp", "tensor"), None), P("dp", "tensor"), P(None, "tensor"))
    return jax.shard_map(
        on_device,
        mesh=mesh,
        in_specs=placed,
        out_specs=(P(("dp", "tensor"), None), P("dp", "tensor")),
        check_vma=False,
    )
```

```python
import functools

import jax
import jax.numpy as jnp
from jax import lax
from jax.experimental import pallas as pl
from jax.experimental.pallas import tpu as pltpu
from jax.sharding import PartitionSpec as P

VMEM = pltpu.CompilerParams(vmem_limit_bytes=56 * 1024 * 1024)
LANES = 128
SUBLANES = 8
STEEP = 127.0
LOW = 2.0**-3.5
SMALLEST = 1e-30


def cost(flops, nbytes):
    return pl.CostEstimate(flops=int(flops), bytes_accessed=int(nbytes), transcendentals=0)


def flip(value, axis, bit):
    pairs = [(i, i ^ bit) for i in range(lax.axis_size(axis))]
    return lax.ppermute(value, axis, pairs)


def from_replica(value, step, swap):
    size = lax.axis_size("dp")
    pairs = [(i, ((i // 2 + step) % (size // 2)) * 2 + (i % 2 ^ swap)) for i in range(size)]
    return lax.ppermute(value, "dp", pairs)


def to_word(value, peak):
    t = LOW + jnp.abs(value) * ((STEEP * LOW) / peak)
    for _ in range(5):
        t = t * t
    return jnp.where(value < 0, -t, t)


def from_word(word, peak):
    t = jnp.exp2(jnp.log2(jnp.abs(word)) * (1.0 / 32.0))
    size = (t - LOW) * (peak * (1.0 / (STEEP * LOW)))
    return jnp.where(word < 0, -size, size)


def block_peak(value):
    top = jnp.maximum(jnp.max(jnp.abs(value)), SMALLEST)
    return top.astype(jnp.bfloat16).astype(jnp.float32)


def split_and_encode(terms_ref, bit, inner, kept_ref, sent_ref):
    n, rows, cols = kept_ref.shape
    for m in range(n):
        base = (m // inner) * 2 * inner + m % inner
        kept_ref[m] = terms_ref[base + bit * inner]
        gone = terms_ref[base + (1 - bit) * inner]
        peak = block_peak(gone)
        sent_ref[m * rows : (m + 1) * rows, :] = to_word(gone, peak).astype(jnp.bfloat16)
        sent_ref[n * rows + m : n * rows + m + 1, :] = jnp.full((1, cols), peak, jnp.bfloat16)
    if n < SUBLANES:
        sent_ref[n * rows + n :, :] = jnp.zeros((SUBLANES - n, cols), jnp.bfloat16)


def decode_and_add(kept_ref, word_ref, terms_ref):
    n, rows, _ = kept_ref.shape
    for m in range(n):
        word = word_ref[m * rows : (m + 1) * rows, :].astype(jnp.float32)
        peak = word_ref[n * rows : n * rows + SUBLANES, :].astype(jnp.float32)[m : m + 1, :]
        terms_ref[m] = kept_ref[m] + from_word(word, peak)


def product_kernel(inner, where_ref, own_ref, near_ref, weight_ref, kept_ref, sent_ref, terms_ref):
    rows = kept_ref.shape[1]
    first = where_ref[0]
    for source, slot in ((own_ref, first), (near_ref, 1 - first)):
        product = lax.dot_general(
            source[...], weight_ref[...], (((1,), (1,)), ((), ())), preferred_element_type=jnp.float32
        )
        half = terms_ref.shape[0] // 2
        for t in range(half):
            terms_ref[slot * half + t] = product[t * rows : (t + 1) * rows, :]
    split_and_encode(terms_ref, where_ref[1], inner, kept_ref, sent_ref)


def products(where, own, near, weight, rows, start, width, tile, inner):
    tokens, hidden = own.shape
    blocks = 2 * tokens // rows
    n = blocks // 2
    core_tiles = weight.shape[0] // 2 // tile
    out_shape = (
        jax.ShapeDtypeStruct((n, rows, width), jnp.float32),
        jax.ShapeDtypeStruct((n * rows + SUBLANES, width), jnp.bfloat16),
    )
    spec = pltpu.PrefetchScalarGridSpec(
        num_scalar_prefetch=1,
        grid=(width // tile,),
        in_specs=[
            pl.BlockSpec((tokens, hidden), lambda i, s: (0, 0)),
            pl.BlockSpec((tokens, hidden), lambda i, s: (0, 0)),
            pl.BlockSpec((tile, hidden), lambda i, s: (s[0] * core_tiles + start // tile + i, 0)),
        ],
        out_specs=[
            pl.BlockSpec((n, rows, tile), lambda i, s: (0, 0, i)),
            pl.BlockSpec((n * rows + SUBLANES, tile), lambda i, s: (0, i)),
        ],
        scratch_shapes=[pltpu.VMEM((blocks, rows, tile), jnp.float32)],
    )
    return pl.pallas_call(
        functools.partial(product_kernel, inner),
        out_shape=out_shape,
        grid_spec=spec,
        compiler_params=VMEM,
        cost_estimate=cost(4 * tokens * hidden * width, 2 * hidden * width),
        name="products",
    )(where, own, near, weight)


def halve_kernel(inner, where_ref, kept_ref, word_ref, next_ref, sent_ref, terms_ref):
    decode_and_add(kept_ref, word_ref, terms_ref)
    split_and_encode(terms_ref, where_ref[0], inner, next_ref, sent_ref)


def halve(bit, kept, word, tile, inner):
    n, rows, width = kept.shape
    m = n // 2
    spec = pltpu.PrefetchScalarGridSpec(
        num_scalar_prefetch=1,
        grid=(width // tile,),
        in_specs=[
            pl.BlockSpec((n, rows, tile), lambda i, s: (0, 0, i)),
            pl.BlockSpec((n * rows + SUBLANES, tile), lambda i, s: (0, i)),
        ],
        out_specs=[
            pl.BlockSpec((m, rows, tile), lambda i, s: (0, 0, i)),
            pl.BlockSpec((m * rows + SUBLANES, tile), lambda i, s: (0, i)),
        ],
        scratch_shapes=[pltpu.VMEM((n, rows, tile), jnp.float32)],
    )
    return pl.pallas_call(
        functools.partial(halve_kernel, inner),
        out_shape=(
            jax.ShapeDtypeStruct((m, rows, width), jnp.float32),
            jax.ShapeDtypeStruct((m * rows + SUBLANES, width), jnp.bfloat16),
        ),
        grid_spec=spec,
        compiler_params=VMEM,
        cost_estimate=cost(1e9, 1e6),
        name="halve",
    )(bit.reshape(1), kept, word)


def finish_kernel(where_ref, kept_ref, word_ref, mine_ref, other_ref, terms_ref):
    decode_and_add(kept_ref, word_ref, terms_ref)
    core = where_ref[0]
    mine_ref[...] = terms_ref[core].astype(jnp.bfloat16)
    other_ref[...] = terms_ref[1 - core].astype(jnp.bfloat16)


def finish(core, kept, word, tile):
    n, rows, width = kept.shape
    shape = jax.ShapeDtypeStruct((rows, width), jnp.bfloat16)
    spec = pltpu.PrefetchScalarGridSpec(
        num_scalar_prefetch=1,
        grid=(width // tile,),
        in_specs=[
            pl.BlockSpec((n, rows, tile), lambda i, s: (0, 0, i)),
            pl.BlockSpec((n * rows + SUBLANES, tile), lambda i, s: (0, i)),
        ],
        out_specs=[pl.BlockSpec((rows, tile), lambda i, s: (0, i))] * 2,
        scratch_shapes=[pltpu.VMEM((n, rows, tile), jnp.float32)],
    )
    return pl.pallas_call(
        finish_kernel,
        out_shape=(shape, shape),
        grid_spec=spec,
        compiler_params=VMEM,
        cost_estimate=cost(5e8, 1e6),
        name="finish",
    )(core.reshape(1), kept, word)


def arrange_kernel(order_ref, *refs):
    for k, ref in enumerate(refs[:-1]):
        refs[-1][0, k] = ref[0]


def arrange(order, grads, rows):
    tokens, hidden = grads[0].shape
    ranks = tokens // rows
    views = [g.reshape(ranks, rows, hidden) for g in grads]
    out = pl.pallas_call(
        arrange_kernel,
        out_shape=jax.ShapeDtypeStruct((ranks, len(grads), rows, hidden), jnp.bfloat16),
        grid_spec=pltpu.PrefetchScalarGridSpec(
            num_scalar_prefetch=1,
            grid=(ranks,),
            in_specs=[pl.BlockSpec((1, rows, hidden), lambda i, s: (s[i], 0, 0))] * len(grads),
            out_specs=pl.BlockSpec((1, len(grads), rows, hidden), lambda i, s: (i, 0, 0, 0)),
        ),
        compiler_params=VMEM,
        cost_estimate=cost(1e9, 7e6),
        name="arrange",
    )(order, *views)
    return out.reshape(ranks * len(grads) * rows, hidden)


def outer_kernel(early_ref, late_ref, grads_ref, *rest):
    out_ref, turned_ref = rest[-2:]
    tokens = early_ref.shape[0]

    @pl.when(pl.program_id(1) == 0)
    def _():
        turned_ref[:, :tokens] = early_ref[...].T
        turned_ref[:, tokens:] = late_ref[...].T

    out_ref[...] = jnp.dot(turned_ref[...], grads_ref[...], preferred_element_type=jnp.float32)


def outer(early, late, grads, total, start, tile, across, into):
    tokens, width = early.shape
    hidden = grads.shape[1]
    operands = [early, late, grads]
    in_specs = [
        pl.BlockSpec((tokens, tile), lambda i, j: (0, i)),
        pl.BlockSpec((tokens, tile), lambda i, j: (0, i)),
        pl.BlockSpec((2 * tokens, across), lambda i, j: (0, j)),
    ]
    aliases = {}
    if into is not None:
        operands.append(into)
        in_specs.append(pl.BlockSpec(memory_space=pl.ANY))
        aliases = {3: 0}
    return pl.pallas_call(
        outer_kernel,
        out_shape=jax.ShapeDtypeStruct((total, hidden), jnp.float32),
        grid=(width // tile, hidden // across),
        in_specs=in_specs,
        out_specs=pl.BlockSpec((tile, across), lambda i, j: (start // tile + i, j)),
        scratch_shapes=[pltpu.VMEM((tile, 2 * tokens), jnp.bfloat16)],
        input_output_aliases=aliases,
        compiler_params=VMEM,
        cost_estimate=cost(4 * tokens * width * hidden, 4 * width * hidden),
        name="outer",
    )(*operands)


def tile_of(width, most):
    for count in range(1, width // LANES + 1):
        if width % count == 0 and width // count % LANES == 0 and width // count <= most:
            return width // count
    return None


def tiled_plan(activations, grad_out, weight):
    replicas, ranks = lax.axis_size("dp"), lax.axis_size("tensor")
    me, rank = lax.axis_index("dp"), lax.axis_index("tensor")
    core = me % 2
    chip = me // 2
    chips = replicas // 2
    rows, features = activations.shape
    steps = [(s, w) for s in range(chips) for w in (0, 1)]
    bits = [1 << k for k in range(ranks.bit_length() - 1)]
    my_bit = {b: (rank // b) % 2 for b in bits}

    near = from_replica(grad_out, 0, 1)
    own_block = features // replicas

    def block_for(step, swap):
        to = ((chip + step) % chips) * 2 + (core ^ swap)
        return lax.dynamic_slice_in_dim(activations, to * own_block, own_block, 1)

    pieces = [block_for(0, 0)]
    pieces += [from_replica(block_for(s, w), s, w) for s, w in steps[1:]]
    local = jnp.concatenate(pieces)

    grads = {(0, 0): grad_out, (0, 1): near}
    for s in range(1, chips):
        grads[s, 0] = from_replica(grad_out, s, 0)
        grads[s, 1] = from_replica(grads[s, 0], 0, 1)

    half = features // 2
    tile = tile_of(half, 384)
    chunks = [(0, half // 2, bits), (half // 2, half // 2, [bits[1], bits[0]] + bits[2:])]
    mine, other = [], []
    for start, width, order in chunks:
        left = list(bits)
        kept = word = None
        for b in order:
            inner = 1 << left.index(b)
            if kept is None:
                where = jnp.stack([core, my_bit[b]]).astype(jnp.int32)
                kept, word = products(where, grad_out, near, weight, rows, start, width, tile, inner)
            else:
                kept, word = halve(my_bit[b].astype(jnp.int32), kept, word, tile, inner)
            left.remove(b)
            word = flip(word, "tensor", b)
        keep, give = finish(core.astype(jnp.int32), kept, word, tile)
        mine.append(keep)
        other.append(from_replica(give, 0, 1))
    mine, other = jnp.concatenate(mine, 1), jnp.concatenate(other, 1)
    input_grad = jnp.concatenate(
        [jnp.where(core == 0, mine, other), jnp.where(core == 0, other, mine)], 1
    )

    relative = [0]
    for b in reversed(bits):
        relative += [r ^ b for r in relative]
    order = (rank ^ jnp.array(relative, jnp.int32)).astype(jnp.int32)
    arranged = arrange(order, [grads[k] for k in steps], rows)
    row_tile = tile_of(own_block, own_block // 3)
    weight_grad = None
    for start, width in ((0, own_block - row_tile), (own_block - row_tile, row_tile)):
        held = local[:, start : start + width]
        for b in reversed(bits):
            came = flip(held, "tensor", b)
            if b != bits[0]:
                held = jnp.concatenate([held, came])
        weight_grad = outer(
            held, came, arranged, own_block, start, row_tile, tile_of(arranged.shape[1], 768), weight_grad
        )
    return (input_grad, weight_grad)


def plain_halves(blocks, mine):
    kept = lax.dynamic_index_in_dim(blocks, mine, 1, keepdims=False)
    sent = lax.dynamic_index_in_dim(blocks, 1 - mine, 1, keepdims=False)
    return kept, sent


def plain_scatter(partial, axis):
    size = lax.axis_size(axis)
    me = lax.axis_index(axis)
    rows, cols = partial.shape
    running = partial.reshape(size, rows // size, cols)
    for bit in [1 << k for k in range(size.bit_length() - 1)]:
        pairs = running.reshape(running.shape[0] // 2, 2, rows // size, cols)
        kept, sent = plain_halves(pairs, (me // bit) % 2)
        running = kept + flip(sent, axis, bit)
    return running[0]


def plain_gather(block, axis):
    size = lax.axis_size(axis)
    me = lax.axis_index(axis)
    held = block[None]
    for bit in reversed([1 << k for k in range(size.bit_length() - 1)]):
        other = flip(held, axis, bit)
        mine = (me // bit) % 2
        low = jnp.where(mine == 0, held, other)
        high = jnp.where(mine == 0, other, held)
        held = jnp.stack([low, high], 1).reshape(2 * held.shape[0], *held.shape[1:])
    return held


def plain_plan(activations, grad_out, weight):
    ranks = lax.axis_size("tensor")
    chips = lax.axis_size("dp") // 2
    me = lax.axis_index("dp")
    chip, core = me // 2, me % 2
    shard_rows, features = activations.shape
    wide = features // chips

    def block_for(step):
        return lax.dynamic_slice_in_dim(activations, ((chip + step) % chips) * wide, wide, 1)

    rows = [block_for(0)] + [from_replica(block_for(k), k, 0) for k in range(1, chips)]
    grads_near = from_replica(grad_out, 0, 1)
    grads_far = [from_replica(grad_out, k, 0) for k in range(1, chips)]
    partial = lax.dot_general(
        grad_out, weight, (((1,), (1,)), ((), ())), preferred_element_type=jnp.float32
    )
    held = plain_gather(jnp.stack(rows), "tensor")
    held = held.transpose(1, 0, 2, 3).reshape(chips * ranks * shard_rows, 2, wide // 2)
    kept, sent = plain_halves(held, core)
    columns = jnp.concatenate([kept, from_replica(sent, 0, 1)])
    grads = jnp.concatenate(
        [grad_out, *grads_far, grads_near, *[from_replica(g, 0, 1) for g in grads_far]]
    )
    input_grad = plain_scatter(partial, "tensor").astype(jnp.bfloat16)
    weight_grad = lax.dot_general(
        columns, grads, (((0,), (0,)), ((), ())), preferred_element_type=jnp.float32
    )
    return (input_grad, weight_grad)


def on_device(activations, grad_out, weight):
    rows, features = activations.shape
    ranks = lax.axis_size("tensor")
    blocks = features // lax.axis_size("dp")
    fits = (
        rows % SUBLANES == 0
        and 4 <= ranks <= SUBLANES
        and blocks % (3 * LANES) == 0
        and grad_out.shape[1] % LANES == 0
    )
    plan = tiled_plan if fits else plain_plan
    return plan(activations, grad_out, weight)


def solution(mesh):
    placed = (P(("dp", "tensor"), None), P("dp", "tensor"), P(None, "tensor"))
    return jax.shard_map(
        on_device,
        mesh=mesh,
        in_specs=placed,
        out_specs=(P(("dp", "tensor"), None), P("dp", "tensor")),
        check_vma=False,
    )
```

```python
import functools

import jax
import jax.numpy as jnp
from jax import lax
from jax.experimental import pallas as pl
from jax.experimental.pallas import tpu as pltpu
from jax.sharding import PartitionSpec as P

LANES = 128
SUBLANES = 8
STEEP = 127.0
LOW = 2.0**-3.5
SMALLEST = 1e-30


def cost(flops, nbytes):
    return pl.CostEstimate(flops=int(flops), bytes_accessed=int(nbytes), transcendentals=0)


def flip(value, axis, bit):
    pairs = [(i, i ^ bit) for i in range(lax.axis_size(axis))]
    return lax.ppermute(value, axis, pairs)


def from_replica(value, step, swap):
    size = lax.axis_size("dp")
    pairs = [(i, ((i // 2 + step) % (size // 2)) * 2 + (i % 2 ^ swap)) for i in range(size)]
    return lax.ppermute(value, "dp", pairs)


def to_word(value, peak):
    t = LOW + jnp.abs(value) * ((STEEP * LOW) / peak)
    for _ in range(5):
        t = t * t
    return jnp.where(value < 0, -t, t)


def from_word(word, peak):
    t = jnp.exp2(jnp.log2(jnp.abs(word)) * (1.0 / 32.0))
    size = (t - LOW) * (peak * (1.0 / (STEEP * LOW)))
    return jnp.where(word < 0, -size, size)


def block_peak(value):
    top = jnp.maximum(jnp.max(jnp.abs(value)), SMALLEST)
    return top.astype(jnp.bfloat16).astype(jnp.float32)


def in_vmem(value):
    return pltpu.with_memory_space_constraint(value, pltpu.VMEM)


def spaces(count, where=pltpu.VMEM):
    return [pl.BlockSpec(memory_space=where)] * count


def limit(mebibytes):
    return pltpu.CompilerParams(vmem_limit_bytes=mebibytes * 1024 * 1024)


def split_and_encode(terms_ref, kept, sent, kept_ref, sent_ref):
    n, rows, cols = kept_ref.shape
    for m in range(n):
        kept_ref[m] = terms_ref[kept[m]]
        gone = terms_ref[sent[m]]
        peak = block_peak(gone)
        sent_ref[m * rows : (m + 1) * rows, :] = to_word(gone, peak).astype(jnp.bfloat16)
        sent_ref[n * rows + m : n * rows + m + 1, :] = jnp.full((1, cols), peak, jnp.bfloat16)
    if n < SUBLANES:
        sent_ref[n * rows + n :, :] = jnp.zeros((SUBLANES - n, cols), jnp.bfloat16)


def decode_and_add(kept_ref, word_ref, terms_ref):
    n, rows, _ = kept_ref.shape
    peaks = word_ref[n * rows : n * rows + SUBLANES, :].astype(jnp.float32)
    for m in range(n):
        word = word_ref[m * rows : (m + 1) * rows, :].astype(jnp.float32)
        terms_ref[m] = kept_ref[m] + from_word(word, peaks[m : m + 1, :])


def prepare_kernel(sources, where_ref, acts_ref, grads_ref, *refs):
    piece_refs, turned_ref, sem = refs[:-2], refs[-2], refs[-1]
    rows, width = piece_refs[0].shape
    copies = []
    for k, ref in enumerate(piece_refs):
        start = pl.multiple_of(where_ref[k] * width, LANES)
        copies.append(pltpu.make_async_copy(acts_ref.at[:, pl.ds(start, width)], ref, sem.at[k]))
    for p in range(sources):
        start = pl.multiple_of(where_ref[len(piece_refs) + p] * rows, SUBLANES)
        copies.append(
            pltpu.make_async_copy(
                grads_ref.at[pl.ds(start, rows), :],
                turned_ref.at[p * rows : (p + 1) * rows, :],
                sem.at[len(piece_refs) + p],
            )
        )
    for copy in copies:
        copy.start()
    for copy in copies:
        copy.wait()


def prepare(where, activations, grads, replicas, ranks):
    rows, features = activations.shape
    width = features // replicas
    out_shape = [pltpu.VMEM((rows, width), jnp.bfloat16)] * replicas
    return pl.pallas_call(
        functools.partial(prepare_kernel, ranks),
        out_shape=(*out_shape, pltpu.VMEM(grads.shape, jnp.bfloat16)),
        grid_spec=pltpu.PrefetchScalarGridSpec(
            num_scalar_prefetch=1,
            grid=(),
            in_specs=spaces(2, pl.ANY),
            out_specs=spaces(replicas + 1),
            scratch_shapes=[pltpu.SemaphoreType.DMA((replicas + ranks,))],
        ),
        compiler_params=limit(4),
        cost_estimate=cost(1e8, 3e6),
        name="prepare",
    )(where, activations, grads)


def product_kernel(start, tile, kept, sent, core_ref, own_ref, near_ref, weight_ref, kept_ref, sent_ref, held_ref, both_ref, terms_ref, sem):
    tokens, hidden = own_ref.shape
    rows, width = kept_ref.shape[1:]
    first = core_ref[0] * (weight_ref.shape[0] // 2) + start
    copies = []
    for i in range(width // tile):
        at = pl.multiple_of(first + i * tile, LANES)
        copies.append(pltpu.make_async_copy(weight_ref.at[pl.ds(at, tile), :], held_ref.at[i], sem.at[i]))
    for copy in copies:
        copy.start()
    both_ref[:tokens, :] = own_ref[...]
    both_ref[tokens:, :] = near_ref[...]
    for i, copy in enumerate(copies):
        copy.wait()
        product = lax.dot_general(
            both_ref[...], held_ref[i], (((1,), (1,)), ((), ())), preferred_element_type=jnp.float32
        )
        for t in range(terms_ref.shape[0]):
            terms_ref[t, :, i * tile : (i + 1) * tile] = product[t * rows : (t + 1) * rows, :]
    split_and_encode(terms_ref, kept, sent, kept_ref, sent_ref)


def products(core, own, near, weight, rows, start, width, tile, kept, sent):
    tokens, hidden = own.shape
    n = tokens // rows
    return pl.pallas_call(
        functools.partial(product_kernel, start, tile, kept, sent),
        out_shape=(
            pltpu.VMEM((n, rows, width), jnp.float32),
            pltpu.VMEM((n * rows + SUBLANES, width), jnp.bfloat16),
        ),
        grid_spec=pltpu.PrefetchScalarGridSpec(
            num_scalar_prefetch=1,
            grid=(),
            in_specs=[*spaces(2), *spaces(1, pl.ANY)],
            out_specs=spaces(2),
            scratch_shapes=[
                pltpu.VMEM((width // tile, tile, hidden), jnp.bfloat16),
                pltpu.VMEM((2 * tokens, hidden), jnp.bfloat16),
                pltpu.VMEM((2 * n, rows, width), jnp.float32),
                pltpu.SemaphoreType.DMA((width // tile,)),
            ],
        ),
        compiler_params=limit(20),
        cost_estimate=cost(4 * tokens * hidden * width, 2 * hidden * width),
        name="products",
    )(core, in_vmem(own), in_vmem(near), weight)


def halve_kernel(kept, sent, kept_ref, word_ref, next_ref, sent_ref, terms_ref):
    decode_and_add(kept_ref, word_ref, terms_ref)
    split_and_encode(terms_ref, kept, sent, next_ref, sent_ref)


def halve(held, word, kept, sent):
    n, rows, width = held.shape
    m = n // 2
    return pl.pallas_call(
        functools.partial(halve_kernel, kept, sent),
        out_shape=(
            pltpu.VMEM((m, rows, width), jnp.float32),
            pltpu.VMEM((m * rows + SUBLANES, width), jnp.bfloat16),
        ),
        in_specs=spaces(2),
        out_specs=spaces(2),
        scratch_shapes=[pltpu.VMEM((n, rows, width), jnp.float32)],
        compiler_params=limit(8),
        cost_estimate=cost(1e9, 1e6),
        name="halve",
    )(in_vmem(held), in_vmem(word))


def finish_kernel(kept_ref, word_ref, mine_ref, other_ref, terms_ref):
    decode_and_add(kept_ref, word_ref, terms_ref)
    mine_ref[...] = terms_ref[0].astype(jnp.bfloat16)
    other_ref[...] = terms_ref[1].astype(jnp.bfloat16)


def finish(held, word):
    n, rows, width = held.shape
    shape = pltpu.VMEM((rows, width), jnp.bfloat16)
    return pl.pallas_call(
        finish_kernel,
        out_shape=(shape, shape),
        in_specs=spaces(2),
        out_specs=spaces(2),
        scratch_shapes=[pltpu.VMEM((n, rows, width), jnp.float32)],
        compiler_params=limit(8),
        cost_estimate=cost(5e8, 1e6),
        name="finish",
    )(in_vmem(held), in_vmem(word))


def outer(early, late, grads, total, start, tile, across, into):
    k, p, rows, width = early.shape
    tokens, hidden = grads.shape
    half = p * rows

    def body(early_ref, late_ref, grads_ref, *rest):
        out_ref, joined_ref, turned_ref = rest[-3:]

        @pl.when(pl.program_id(1) == 0)
        def _():
            for i in range(width // tile):

                @pl.when(pl.program_id(0) == i)
                def _():
                    cols = slice(i * tile, (i + 1) * tile)
                    for j in range(k):
                        base = 2 * j * half
                        joined_ref[base : base + half, :] = early_ref[j * half : (j + 1) * half, cols]
                        joined_ref[base + half : base + 2 * half, :] = late_ref[j * half : (j + 1) * half, cols]

            turned_ref[...] = joined_ref[...].T

        for j in range(hidden // across):

            @pl.when(pl.program_id(1) == j)
            def _():
                out_ref[...] = jnp.dot(
                    turned_ref[...], grads_ref[:, j * across : (j + 1) * across], preferred_element_type=jnp.float32
                )

    operands = [in_vmem(early.reshape(k * half, width)), in_vmem(late.reshape(k * half, width)), in_vmem(grads)]
    in_specs = spaces(3)
    aliases = {}
    if into is not None:
        operands.append(into)
        in_specs = in_specs + spaces(1, pl.ANY)
        aliases = {3: 0}
    return pl.pallas_call(
        body,
        out_shape=jax.ShapeDtypeStruct((total, hidden), jnp.float32),
        grid=(width // tile, hidden // across),
        in_specs=in_specs,
        out_specs=pl.BlockSpec((tile, across), lambda i, j: (start // tile + i, j)),
        scratch_shapes=[pltpu.VMEM((tokens, tile), jnp.bfloat16), pltpu.VMEM((tile, tokens), jnp.bfloat16)],
        input_output_aliases=aliases,
        compiler_params=limit(16),
        cost_estimate=cost(2 * tokens * width * hidden, 4 * width * hidden),
        name="outer",
    )(*operands)


def tile_of(width, most):
    for count in range(1, width // LANES + 1):
        if width % count == 0 and width // count % LANES == 0 and width // count <= most:
            return width // count
    return None


def split_lists(labels, bit):
    kept = [i for i, (_, r) in enumerate(labels) if not r & bit]
    sent = [labels.index((labels[i][0], labels[i][1] ^ bit)) for i in kept]
    return kept, sent


def tiled_plan(activations, grad_out, weight):
    replicas, ranks = lax.axis_size("dp"), lax.axis_size("tensor")
    me, rank = lax.axis_index("dp"), lax.axis_index("tensor")
    core, chip, chips = me % 2, me // 2, replicas // 2
    rows, features = activations.shape
    steps = [(s, w) for s in range(chips) for w in (0, 1)]
    bits = [1 << k for k in range(ranks.bit_length() - 1)]
    relative = [0]
    for b in reversed(bits):
        relative += [r ^ b for r in relative]

    where = jnp.stack(
        [((chip + s) % chips) * 2 + (core ^ w) for s, w in steps] + [rank ^ r for r in relative]
    ).astype(jnp.int32)
    *blocks, own = prepare(where, activations, grad_out, replicas, ranks)
    near = from_replica(own, 0, 1)
    pieces = [blocks[0]] + [from_replica(x, s, w) for x, (s, w) in zip(blocks[1:], steps[1:])]
    local = jnp.stack(pieces)[:, None]

    grads = [own, near]
    for s in range(1, chips):
        grads.append(from_replica(own, s, 0))
        grads.append(from_replica(grads[-1], 0, 1))

    half = features // 2
    chunks = [(0, half // 2, bits), (half // 2, half // 2, [bits[1], bits[0]] + bits[2:])]
    core_at = core.astype(jnp.int32).reshape(1)
    mine, other = [], []
    for start, width, order in chunks:
        labels = [(c, r) for c in (0, 1) for r in relative]
        held = word = None
        for b in order:
            kept, sent = split_lists(labels, b)
            if held is None:
                held, word = products(
                    core_at, own, near, weight, rows, start, width, tile_of(width, 384), kept, sent
                )
            else:
                held, word = halve(held, word, kept, sent)
            labels = [labels[i] for i in kept]
            word = flip(word, "tensor", b)
        keep, give = finish(held, word)
        mine.append(keep)
        other.append(from_replica(give, 0, 1))
    mine, other = jnp.concatenate(mine, 1), jnp.concatenate(other, 1)
    input_grad = jnp.concatenate(
        [jnp.where(core == 0, mine, other), jnp.where(core == 0, other, mine)], 1
    )

    own_block = features // replicas
    all_grads = jnp.concatenate(grads)
    row_tile = tile_of(own_block, own_block // 3)
    weight_grad = None
    for start, width in ((0, own_block - row_tile), (own_block - row_tile, row_tile)):
        held = local[..., start : start + width]
        for b in reversed(bits):
            came = flip(held, "tensor", b)
            if b != bits[0]:
                held = jnp.concatenate([held, came], 1)
        weight_grad = outer(
            held, came, all_grads, own_block, start, row_tile, tile_of(grad_out.shape[1], 768), weight_grad
        )
    return (input_grad, weight_grad)


def plain_halves(blocks, mine):
    kept = lax.dynamic_index_in_dim(blocks, mine, 1, keepdims=False)
    sent = lax.dynamic_index_in_dim(blocks, 1 - mine, 1, keepdims=False)
    return kept, sent


def plain_scatter(partial, axis):
    size = lax.axis_size(axis)
    me = lax.axis_index(axis)
    rows, cols = partial.shape
    running = partial.reshape(size, rows // size, cols)
    for bit in [1 << k for k in range(size.bit_length() - 1)]:
        pairs = running.reshape(running.shape[0] // 2, 2, rows // size, cols)
        kept, sent = plain_halves(pairs, (me // bit) % 2)
        running = kept + flip(sent, axis, bit)
    return running[0]


def plain_gather(block, axis):
    size = lax.axis_size(axis)
    me = lax.axis_index(axis)
    held = block[None]
    for bit in reversed([1 << k for k in range(size.bit_length() - 1)]):
        other = flip(held, axis, bit)
        mine = (me // bit) % 2
        low = jnp.where(mine == 0, held, other)
        high = jnp.where(mine == 0, other, held)
        held = jnp.stack([low, high], 1).reshape(2 * held.shape[0], *held.shape[1:])
    return held


def plain_plan(activations, grad_out, weight):
    ranks = lax.axis_size("tensor")
    chips = lax.axis_size("dp") // 2
    me = lax.axis_index("dp")
    chip, core = me // 2, me % 2
    shard_rows, features = activations.shape
    wide = features // chips

    def block_for(step):
        return lax.dynamic_slice_in_dim(activations, ((chip + step) % chips) * wide, wide, 1)

    rows = [block_for(0)] + [from_replica(block_for(k), k, 0) for k in range(1, chips)]
    grads_near = from_replica(grad_out, 0, 1)
    grads_far = [from_replica(grad_out, k, 0) for k in range(1, chips)]
    partial = lax.dot_general(
        grad_out, weight, (((1,), (1,)), ((), ())), preferred_element_type=jnp.float32
    )
    held = plain_gather(jnp.stack(rows), "tensor")
    held = held.transpose(1, 0, 2, 3).reshape(chips * ranks * shard_rows, 2, wide // 2)
    kept, sent = plain_halves(held, core)
    columns = jnp.concatenate([kept, from_replica(sent, 0, 1)])
    grads = jnp.concatenate(
        [grad_out, *grads_far, grads_near, *[from_replica(g, 0, 1) for g in grads_far]]
    )
    input_grad = plain_scatter(partial, "tensor").astype(jnp.bfloat16)
    weight_grad = lax.dot_general(
        columns, grads, (((0,), (0,)), ((), ())), preferred_element_type=jnp.float32
    )
    return (input_grad, weight_grad)


def on_device(activations, grad_out, weight):
    rows, features = activations.shape
    ranks = lax.axis_size("tensor")
    blocks = features // lax.axis_size("dp")
    fits = (
        rows % SUBLANES == 0
        and 4 <= ranks <= SUBLANES
        and blocks % (3 * LANES) == 0
        and grad_out.shape[1] % LANES == 0
    )
    plan = tiled_plan if fits else plain_plan
    return plan(activations, grad_out, weight)


def solution(mesh):
    placed = (P(("dp", "tensor"), None), P("dp", "tensor"), P(None, "tensor"))
    return jax.shard_map(
        on_device,
        mesh=mesh,
        in_specs=placed,
        out_specs=(P(("dp", "tensor"), None), P("dp", "tensor")),
        check_vma=False,
    )
```

```python
import functools

import jax
import jax.numpy as jnp
from jax import lax
from jax.experimental import pallas as pl
from jax.experimental.pallas import tpu as pltpu
from jax.sharding import PartitionSpec as P

LANES = 128
SUBLANES = 8
SUM_A = (0, 1, 2)
SUM_B = (0, 1, 2)
SPREAD_A = (2, 1, 0)
SPREAD_B = (2, 1, 0)
STEEP = 127.0
LOW = 2.0**-3.5
SMALLEST = 1e-30


def cost(flops, nbytes):
    return pl.CostEstimate(flops=int(flops), bytes_accessed=int(nbytes), transcendentals=0)


def flip(value, axis, bit):
    pairs = [(i, i ^ bit) for i in range(lax.axis_size(axis))]
    return lax.ppermute(value, axis, pairs)


def from_replica(value, step, swap):
    size = lax.axis_size("dp")
    pairs = [(i, ((i // 2 + step) % (size // 2)) * 2 + (i % 2 ^ swap)) for i in range(size)]
    return lax.ppermute(value, "dp", pairs)


def to_word(value, peak):
    t = LOW + jnp.abs(value) * ((STEEP * LOW) / peak)
    for _ in range(5):
        t = t * t
    return jnp.where(value < 0, -t, t)


def from_word(word, peak):
    t = jnp.exp2(jnp.log2(jnp.abs(word)) * (1.0 / 32.0))
    size = (t - LOW) * (peak * (1.0 / (STEEP * LOW)))
    return jnp.where(word < 0, -size, size)


def block_peak(value):
    top = jnp.maximum(jnp.max(jnp.abs(value)), SMALLEST)
    return top.astype(jnp.bfloat16).astype(jnp.float32)


def in_vmem(value):
    return pltpu.with_memory_space_constraint(value, pltpu.VMEM)


def in_hbm(value):
    return pltpu.with_memory_space_constraint(value, pltpu.HBM)


def spaces(count, where=pltpu.VMEM):
    return [pl.BlockSpec(memory_space=where)] * count


def limit(mebibytes):
    return pltpu.CompilerParams(vmem_limit_bytes=mebibytes * 1024 * 1024)


def split_and_encode(terms_ref, kept, sent, kept_ref, sent_ref):
    n, rows, cols = kept_ref.shape
    for m in range(n):
        kept_ref[m] = terms_ref[kept[m]]
        gone = terms_ref[sent[m]]
        peak = block_peak(gone)
        sent_ref[m * rows : (m + 1) * rows, :] = to_word(gone, peak).astype(jnp.bfloat16)
        sent_ref[n * rows + m : n * rows + m + 1, :] = jnp.full((1, cols), peak, jnp.bfloat16)
    if n < SUBLANES:
        sent_ref[n * rows + n :, :] = jnp.zeros((SUBLANES - n, cols), jnp.bfloat16)


def decode_and_add(kept_ref, word_ref, terms_ref):
    n, rows, _ = kept_ref.shape
    peaks = word_ref[n * rows : n * rows + SUBLANES, :].astype(jnp.float32)
    for m in range(n):
        word = word_ref[m * rows : (m + 1) * rows, :].astype(jnp.float32)
        terms_ref[m] = kept_ref[m] + from_word(word, peaks[m : m + 1, :])


def relatives(ranks):
    found = [0]
    for b in reversed(bits_of(ranks)):
        found += [r ^ b for r in found]
    return found


def bits_of(size):
    return [1 << k for k in range(size.bit_length() - 1)]


def replica_steps(replicas):
    return [(s, w) for s in range(replicas // 2) for w in (0, 1)]


def prepare_kernel(acts_ref, grads_ref, *refs):
    piece_refs, turned_ref, sem = refs[:-2], refs[-2], refs[-1]
    rows, width = piece_refs[0].shape
    replicas = len(piece_refs)
    me, rank = lax.axis_index("dp"), lax.axis_index("tensor")
    copies = []
    for p, r in enumerate(relatives(turned_ref.shape[0] // rows)):
        start = pl.multiple_of(lax.bitwise_xor(rank, jnp.int32(r)) * rows, SUBLANES)
        copies.append(
            pltpu.make_async_copy(
                grads_ref.at[pl.ds(start, rows), :], turned_ref.at[p * rows : (p + 1) * rows, :], sem.at[p]
            )
        )
    for (s, w), ref in zip(replica_steps(replicas), piece_refs):
        chip = lax.rem(lax.div(me, 2) + s, replicas // 2)
        to = chip * 2 + lax.bitwise_xor(lax.rem(me, 2), jnp.int32(w))
        start = pl.multiple_of(to * width, LANES)
        copies.append(pltpu.make_async_copy(acts_ref.at[:, pl.ds(start, width)], ref, sem.at[len(copies)]))
    for copy in copies:
        copy.start()
    for copy in copies:
        copy.wait()


def prepare(activations, grads, replicas, ranks):
    rows, features = activations.shape
    width = features // replicas
    out_shape = [pltpu.VMEM((rows, width), jnp.bfloat16)] * replicas
    return pl.pallas_call(
        prepare_kernel,
        out_shape=(*out_shape, pltpu.VMEM(grads.shape, jnp.bfloat16)),
        in_specs=spaces(2, pltpu.HBM),
        out_specs=tuple(spaces(replicas + 1)),
        scratch_shapes=[pltpu.SemaphoreType.DMA((replicas + ranks,))],
        compiler_params=limit(4),
        cost_estimate=cost(1e8, 3e6),
        name="prepare",
    )(in_hbm(activations), in_hbm(grads))


def copy_kernel(plan, *refs):
    for source, source_at, target, target_at in plan:
        refs[target][target_at] = refs[source][source_at]


def arrange(arrays, shapes, plan):
    count = len(arrays)
    found = pl.pallas_call(
        functools.partial(copy_kernel, [(i, at, count + o, to) for i, at, o, to in plan]),
        out_shape=tuple(pltpu.VMEM(shape, jnp.bfloat16) for shape in shapes),
        in_specs=spaces(count),
        out_specs=tuple(spaces(len(shapes))),
        compiler_params=limit(4),
        cost_estimate=cost(1e8, 1e6),
        name="arrange",
    )(*[in_vmem(x) for x in arrays])
    return found


def joined(first, second):
    k, p, rows, width = first.shape
    every = slice(None)
    return arrange(
        [first, second],
        [(k, 2 * p, rows, width)],
        [(0, (every,), 0, (every, slice(0, p))), (1, (every,), 0, (every, slice(p, 2 * p)))],
    )[0]


def product_kernel(start, tile, kept, sent, own_ref, near_ref, weight_ref, kept_ref, sent_ref, held_ref, both_ref, terms_ref, sem):
    tokens, _ = own_ref.shape
    rows, width = kept_ref.shape[1:]
    first = lax.rem(lax.axis_index("dp"), 2) * (weight_ref.shape[0] // 2) + start
    copies = []
    for i in range(width // tile):
        at = pl.multiple_of(first + i * tile, LANES)
        copies.append(pltpu.make_async_copy(weight_ref.at[pl.ds(at, tile), :], held_ref.at[i], sem.at[i]))
    for copy in copies:
        copy.start()
    both_ref[:tokens, :] = own_ref[...]
    both_ref[tokens:, :] = near_ref[...]
    for i, copy in enumerate(copies):
        copy.wait()
        product = lax.dot_general(
            both_ref[...], held_ref[i], (((1,), (1,)), ((), ())), preferred_element_type=jnp.float32
        )
        for t in range(terms_ref.shape[0]):
            terms_ref[t, :, i * tile : (i + 1) * tile] = product[t * rows : (t + 1) * rows, :]
    split_and_encode(terms_ref, kept, sent, kept_ref, sent_ref)


def products(own, near, weight, rows, start, width, tile, kept, sent):
    tokens, hidden = own.shape
    n = tokens // rows
    return pl.pallas_call(
        functools.partial(product_kernel, start, tile, kept, sent),
        out_shape=(
            pltpu.VMEM((n, rows, width), jnp.float32),
            pltpu.VMEM((n * rows + SUBLANES, width), jnp.bfloat16),
        ),
        in_specs=[*spaces(2), *spaces(1, pltpu.HBM)],
        out_specs=tuple(spaces(2)),
        scratch_shapes=[
            pltpu.VMEM((width // tile, tile, hidden), jnp.bfloat16),
            pltpu.VMEM((2 * tokens, hidden), jnp.bfloat16),
            pltpu.VMEM((2 * n, rows, width), jnp.float32),
            pltpu.SemaphoreType.DMA((width // tile,)),
        ],
        compiler_params=limit(14),
        cost_estimate=cost(4 * tokens * hidden * width, 2 * hidden * width),
        name="products",
    )(in_vmem(own), in_vmem(near), in_hbm(weight))


def halve_kernel(kept, sent, kept_ref, word_ref, next_ref, sent_ref, terms_ref):
    decode_and_add(kept_ref, word_ref, terms_ref)
    split_and_encode(terms_ref, kept, sent, next_ref, sent_ref)


def halve(held, word, kept, sent):
    n, rows, width = held.shape
    m = n // 2
    return pl.pallas_call(
        functools.partial(halve_kernel, kept, sent),
        out_shape=(
            pltpu.VMEM((m, rows, width), jnp.float32),
            pltpu.VMEM((m * rows + SUBLANES, width), jnp.bfloat16),
        ),
        in_specs=spaces(2),
        out_specs=spaces(2),
        scratch_shapes=[pltpu.VMEM((n, rows, width), jnp.float32)],
        compiler_params=limit(5),
        cost_estimate=cost(1e9, 1e6),
        name="halve",
    )(in_vmem(held), in_vmem(word))


def finish_kernel(kept_ref, word_ref, mine_ref, other_ref, terms_ref):
    decode_and_add(kept_ref, word_ref, terms_ref)
    mine_ref[...] = terms_ref[0].astype(jnp.bfloat16)
    other_ref[...] = terms_ref[1].astype(jnp.bfloat16)


def finish(held, word):
    n, rows, width = held.shape
    shape = pltpu.VMEM((rows, width), jnp.bfloat16)
    return pl.pallas_call(
        finish_kernel,
        out_shape=(shape, shape),
        in_specs=spaces(2),
        out_specs=spaces(2),
        scratch_shapes=[pltpu.VMEM((n, rows, width), jnp.float32)],
        compiler_params=limit(5),
        cost_estimate=cost(5e8, 1e6),
        name="finish",
    )(in_vmem(held), in_vmem(word))


def outer(early, late, moves, grads, total, start, tile, across, into, pieces):
    width = early.shape[1]
    tokens, hidden = grads.shape
    count = len(pieces)
    steps = (width // tile, hidden // across)

    def body(*refs):
        early_ref, late_ref, grads_ref = refs[:3]
        piece_refs = refs[3 : 3 + count]
        out_ref = refs[3 + count + (into is not None)]
        joined_ref, turned_ref = refs[-3:-1]
        i, j = pl.program_id(0), pl.program_id(1)
        copies = []
        if count:
            whole_ref, sem = refs[-4], refs[-1]
            core = lax.rem(lax.axis_index("dp"), 2)
            half = whole_ref.shape[1] // 2
            at = 0
            for c, ref in enumerate(piece_refs):
                side = core if c < count // 2 else 1 - core
                at = 0 if c == count // 2 else at
                columns = pl.ds(pl.multiple_of(side * half + at, LANES), ref.shape[1])
                copies.append(pltpu.make_async_copy(ref, whole_ref.at[:, columns], sem.at[c]))
                at += ref.shape[1]

            @pl.when((i == 0) & (j == 0))
            def _():
                for copy in copies:
                    copy.start()

        for row in range(steps[0]):

            @pl.when((j == 0) & (i == row))
            def _():
                cols = slice(row * tile, (row + 1) * tile)
                for is_late, source, target, rows in moves:
                    ref = late_ref if is_late else early_ref
                    joined_ref[target : target + rows, :] = ref[source : source + rows, cols]

        @pl.when(j == 0)
        def _():
            turned_ref[...] = joined_ref[...].T

        for column in range(steps[1]):

            @pl.when(j == column)
            def _():
                out_ref[...] = jnp.dot(
                    turned_ref[...],
                    grads_ref[:, column * across : (column + 1) * across],
                    preferred_element_type=jnp.float32,
                )

        if count:

            @pl.when((i == steps[0] - 1) & (j == steps[1] - 1))
            def _():
                for copy in copies:
                    copy.wait()

    operands = [in_vmem(x) for x in (early, late, grads, *pieces)]
    in_specs = spaces(len(operands))
    aliases = {}
    if into is not None:
        aliases = {len(operands): 0}
        operands.append(in_hbm(into))
        in_specs = in_specs + spaces(1, pltpu.HBM)
    out_shape = [jax.ShapeDtypeStruct((total, hidden), jnp.float32)]
    out_specs = [pl.BlockSpec((tile, across), lambda i, j: (start // tile + i, j))]
    if count:
        columns = sum(x.shape[1] for x in pieces)
        out_shape.append(jax.ShapeDtypeStruct((pieces[0].shape[0], columns), jnp.bfloat16))
        out_specs += spaces(1, pltpu.HBM)
    return pl.pallas_call(
        body,
        out_shape=tuple(out_shape),
        grid=steps,
        in_specs=in_specs,
        out_specs=tuple(out_specs),
        scratch_shapes=[
            pltpu.VMEM((tokens, tile), jnp.bfloat16),
            pltpu.VMEM((tile, tokens), jnp.bfloat16),
            pltpu.SemaphoreType.DMA((max(count, 1),)),
        ],
        input_output_aliases=aliases,
        compiler_params=limit(10),
        cost_estimate=cost(2 * tokens * width * hidden, 4 * width * hidden),
        name="outer",
    )(*operands)


def row_moves(names, order, replicas, rows):
    half = len(names) // 2
    moves = []
    for k in range(replicas):
        for place, r in enumerate(order):
            i = names.index(r)
            late = i >= half
            source = (k * half + i % half) * rows
            target = (k * len(order) + place) * rows
            if moves and moves[-1][0] == late and moves[-1][1] + moves[-1][3] == source:
                was = moves.pop()
                moves.append((late, was[1], was[2], was[3] + rows))
            else:
                moves.append((late, source, target, rows))
    return moves


def tile_of(width, most):
    for count in range(1, width // LANES + 1):
        if width % count == 0 and width // count % LANES == 0 and width // count <= most:
            return width // count
    return None


def split_lists(labels, bit):
    kept = [i for i, (_, r) in enumerate(labels) if not r & bit]
    sent = [labels.index((labels[i][0], labels[i][1] ^ bit)) for i in kept]
    return kept, sent


def tiled_plan(activations, grad_out, weight):
    replicas, ranks = lax.axis_size("dp"), lax.axis_size("tensor")
    chips = replicas // 2
    rows, features = activations.shape
    own_block = features // replicas
    steps = replica_steps(replicas)
    bits = bits_of(ranks)
    relative = relatives(ranks)
    every = slice(None)

    *blocks, own = prepare(activations, grad_out, replicas, ranks)
    near = from_replica(own, 0, 1)
    pieces = [blocks[0]]
    for k in range(1, len(steps)):
        pieces.append(from_replica(blocks[k], *steps[k]))

    row_tile = tile_of(own_block, own_block // 3)
    cuts = {"a": (0, own_block - row_tile), "b": (own_block - row_tile, row_tile)}
    gathered = arrange(
        pieces,
        [(len(steps), 1, rows, width) for _, width in cuts.values()],
        [
            (k, (every, slice(start, start + width)), c, (k, 0))
            for k in range(len(steps))
            for c, (start, width) in enumerate(cuts.values())
        ],
    )

    grads = [own, near]
    for s in range(1, chips):
        grads.append(from_replica(own, s, 0))
        grads.append(from_replica(grads[-1], 0, 1))
    tokens, hidden = grad_out.shape
    (all_grads,) = arrange(
        grads,
        [(len(grads) * tokens, hidden)],
        [(k, (every,), 0, (slice(k * tokens, (k + 1) * tokens),)) for k in range(len(grads))],
    )

    half = features // 2
    chunks = {"a": (0, half // 2, SUM_A), "b": (half // 2, half // 2, SUM_B)}
    mine, other = [], []
    for (start, width, places) in chunks.values():
        labels = [(c, r) for c in (0, 1) for r in relative]
        for i, place in enumerate(places):
            b = bits[place]
            kept, sent = split_lists(labels, b)
            if i == 0:
                held, word = products(own, near, weight, rows, start, width, tile_of(width, 384), kept, sent)
            else:
                held, word = halve(held, word, kept, sent)
            labels = [labels[i] for i in kept]
            word = flip(word, "tensor", b)
        keep, give = finish(held, word)
        mine.append(keep)
        other.append(from_replica(give, 0, 1))
    weight_grad = None
    for held, (name, (start, width)), places in zip(gathered, cuts.items(), (SPREAD_A, SPREAD_B)):
        names = [0]
        for i, place in enumerate(places):
            came = flip(held, "tensor", bits[place])
            names += [r ^ bits[place] for r in names]
            if i < len(bits) - 1:
                held = joined(held, came)
        moves = row_moves(names, relative, replicas, rows)
        flat = (replicas * len(names) // 2 * rows, width)
        weight_grad, *rest = outer(
            held.reshape(flat),
            came.reshape(flat),
            moves,
            all_grads,
            own_block,
            start,
            row_tile,
            tile_of(hidden, 768),
            weight_grad,
            mine + other if name == "b" else [],
        )
    return (rest[0], weight_grad)


def plain_halves(blocks, mine):
    kept = lax.dynamic_index_in_dim(blocks, mine, 1, keepdims=False)
    sent = lax.dynamic_index_in_dim(blocks, 1 - mine, 1, keepdims=False)
    return kept, sent


def plain_scatter(partial, axis):
    size = lax.axis_size(axis)
    me = lax.axis_index(axis)
    rows, cols = partial.shape
    running = partial.reshape(size, rows // size, cols)
    for bit in [1 << k for k in range(size.bit_length() - 1)]:
        pairs = running.reshape(running.shape[0] // 2, 2, rows // size, cols)
        kept, sent = plain_halves(pairs, (me // bit) % 2)
        running = kept + flip(sent, axis, bit)
    return running[0]


def plain_gather(block, axis):
    size = lax.axis_size(axis)
    me = lax.axis_index(axis)
    held = block[None]
    for bit in reversed([1 << k for k in range(size.bit_length() - 1)]):
        other = flip(held, axis, bit)
        mine = (me // bit) % 2
        low = jnp.where(mine == 0, held, other)
        high = jnp.where(mine == 0, other, held)
        held = jnp.stack([low, high], 1).reshape(2 * held.shape[0], *held.shape[1:])
    return held


def plain_plan(activations, grad_out, weight):
    ranks = lax.axis_size("tensor")
    chips = lax.axis_size("dp") // 2
    me = lax.axis_index("dp")
    chip, core = me // 2, me % 2
    shard_rows, features = activations.shape
    wide = features // chips

    def block_for(step):
        return lax.dynamic_slice_in_dim(activations, ((chip + step) % chips) * wide, wide, 1)

    rows = [block_for(0)] + [from_replica(block_for(k), k, 0) for k in range(1, chips)]
    grads_near = from_replica(grad_out, 0, 1)
    grads_far = [from_replica(grad_out, k, 0) for k in range(1, chips)]
    partial = lax.dot_general(
        grad_out, weight, (((1,), (1,)), ((), ())), preferred_element_type=jnp.float32
    )
    held = plain_gather(jnp.stack(rows), "tensor")
    held = held.transpose(1, 0, 2, 3).reshape(chips * ranks * shard_rows, 2, wide // 2)
    kept, sent = plain_halves(held, core)
    columns = jnp.concatenate([kept, from_replica(sent, 0, 1)])
    grads = jnp.concatenate(
        [grad_out, *grads_far, grads_near, *[from_replica(g, 0, 1) for g in grads_far]]
    )
    input_grad = plain_scatter(partial, "tensor").astype(jnp.bfloat16)
    weight_grad = lax.dot_general(
        columns, grads, (((0,), (0,)), ((), ())), preferred_element_type=jnp.float32
    )
    return (input_grad, weight_grad)


def on_device(activations, grad_out, weight):
    rows, features = activations.shape
    ranks = lax.axis_size("tensor")
    blocks = features // lax.axis_size("dp")
    fits = (
        rows % SUBLANES == 0
        and 4 <= ranks <= SUBLANES
        and blocks % (3 * LANES) == 0
        and grad_out.shape[1] % LANES == 0
    )
    plan = tiled_plan if fits else plain_plan
    return plan(activations, grad_out, weight)


def solution(mesh):
    placed = (P(("dp", "tensor"), None), P("dp", "tensor"), P(None, "tensor"))
    return jax.shard_map(
        on_device,
        mesh=mesh,
        in_specs=placed,
        out_specs=(P(("dp", "tensor"), None), P("dp", "tensor")),
        check_vma=False,
    )
```

```python
import functools

import jax
import jax.numpy as jnp
from jax import lax
from jax.experimental import pallas as pl
from jax.experimental.pallas import tpu as pltpu
from jax.sharding import PartitionSpec as P

LANES = 128
SUBLANES = 8
SUM_A = (0, 1, 2)
SUM_B = (0, 1, 2)
OUT_CHUNKS = 2
STEEP = 127.0
LOW = 2.0**-3.5
SMALLEST = 1e-30


def cost(flops, nbytes):
    return pl.CostEstimate(flops=int(flops), bytes_accessed=int(nbytes), transcendentals=0)


def flip(value, axis, bit):
    pairs = [(i, i ^ bit) for i in range(lax.axis_size(axis))]
    return lax.ppermute(value, axis, pairs)


def from_replica(value, step, swap):
    size = lax.axis_size("dp")
    pairs = [(i, ((i // 2 + step) % (size // 2)) * 2 + (i % 2 ^ swap)) for i in range(size)]
    return lax.ppermute(value, "dp", pairs)


def to_word(value, peak):
    t = LOW + jnp.abs(value) * ((STEEP * LOW) / peak)
    for _ in range(5):
        t = t * t
    return jnp.where(value < 0, -t, t)


def from_word(word, peak):
    t = jnp.exp2(jnp.log2(jnp.abs(word)) * (1.0 / 32.0))
    size = (t - LOW) * (peak * (1.0 / (STEEP * LOW)))
    return jnp.where(word < 0, -size, size)


def block_peak(value):
    top = jnp.maximum(jnp.max(jnp.abs(value)), SMALLEST)
    return top.astype(jnp.bfloat16).astype(jnp.float32)


def in_vmem(value):
    return pltpu.with_memory_space_constraint(value, pltpu.VMEM)


def in_hbm(value):
    return pltpu.with_memory_space_constraint(value, pltpu.HBM)


def spaces(count, where=pltpu.VMEM):
    return [pl.BlockSpec(memory_space=where)] * count


def limit(mebibytes):
    return pltpu.CompilerParams(vmem_limit_bytes=mebibytes * 1024 * 1024)


def split_and_encode(terms_ref, kept, sent, kept_ref, sent_ref, start=0, width=None):
    n, rows, cols = kept_ref.shape
    width = cols if width is None else width
    here = slice(start, start + width)
    for m in range(n):
        kept_ref[m, :, here] = terms_ref[kept[m], :, here]
        gone = terms_ref[sent[m], :, here]
        peak = block_peak(gone)
        sent_ref[m * rows : (m + 1) * rows, here] = to_word(gone, peak).astype(jnp.bfloat16)
        sent_ref[n * rows + m : n * rows + m + 1, here] = jnp.full((1, width), peak, jnp.bfloat16)
    if n < SUBLANES:
        sent_ref[n * rows + n :, here] = jnp.zeros((SUBLANES - n, width), jnp.bfloat16)


def decode_and_add(kept_ref, word_ref, terms_ref):
    n, rows, _ = kept_ref.shape
    peaks = word_ref[n * rows : n * rows + SUBLANES, :].astype(jnp.float32)
    for m in range(n):
        word = word_ref[m * rows : (m + 1) * rows, :].astype(jnp.float32)
        terms_ref[m] = kept_ref[m] + from_word(word, peaks[m : m + 1, :])


def relatives(ranks):
    found = [0]
    for b in reversed(bits_of(ranks)):
        found += [r ^ b for r in found]
    return found


def bits_of(size):
    return [1 << k for k in range(size.bit_length() - 1)]


def replica_steps(replicas):
    return [(s, w) for s in range(replicas // 2) for w in (0, 1)]


def prepare_kernel(acts_ref, grads_ref, *refs):
    piece_refs, turned_ref, sem = refs[:-2], refs[-2], refs[-1]
    rows, width = piece_refs[0].shape
    replicas = len(piece_refs)
    me, rank = lax.axis_index("dp"), lax.axis_index("tensor")
    copies = []
    for p, r in enumerate(relatives(turned_ref.shape[0] // rows)):
        start = pl.multiple_of(lax.bitwise_xor(rank, jnp.int32(r)) * rows, SUBLANES)
        copies.append(
            pltpu.make_async_copy(
                grads_ref.at[pl.ds(start, rows), :], turned_ref.at[p * rows : (p + 1) * rows, :], sem.at[p]
            )
        )
    for (s, w), ref in zip(replica_steps(replicas), piece_refs):
        chip = lax.rem(lax.div(me, 2) + s, replicas // 2)
        to = chip * 2 + lax.bitwise_xor(lax.rem(me, 2), jnp.int32(w))
        start = pl.multiple_of(to * width, LANES)
        copies.append(pltpu.make_async_copy(acts_ref.at[:, pl.ds(start, width)], ref, sem.at[len(copies)]))
    for copy in copies:
        copy.start()
    for copy in copies:
        copy.wait()


def prepare(activations, grads, replicas, ranks):
    rows, features = activations.shape
    width = features // replicas
    out_shape = [pltpu.VMEM((rows, width), jnp.bfloat16)] * replicas
    return pl.pallas_call(
        prepare_kernel,
        out_shape=(*out_shape, pltpu.VMEM(grads.shape, jnp.bfloat16)),
        in_specs=spaces(2, pltpu.HBM),
        out_specs=tuple(spaces(replicas + 1)),
        scratch_shapes=[pltpu.SemaphoreType.DMA((replicas + ranks,))],
        compiler_params=limit(4),
        cost_estimate=cost(1e8, 3e6),
        name="prepare",
    )(in_hbm(activations), in_hbm(grads))


def copy_kernel(plan, *refs):
    for source, source_at, target, target_at in plan:
        refs[target][target_at] = refs[source][source_at]


def arrange(arrays, shapes, plan):
    count = len(arrays)
    found = pl.pallas_call(
        functools.partial(copy_kernel, [(i, at, count + o, to) for i, at, o, to in plan]),
        out_shape=tuple(pltpu.VMEM(shape, jnp.bfloat16) for shape in shapes),
        in_specs=spaces(count),
        out_specs=tuple(spaces(len(shapes))),
        compiler_params=limit(4),
        cost_estimate=cost(1e8, 1e6),
        name="arrange",
    )(*[in_vmem(x) for x in arrays])
    return found


def joined(first, second):
    k, p, rows, width = first.shape
    every = slice(None)
    return arrange(
        [first, second],
        [(k, 2 * p, rows, width)],
        [(0, (every,), 0, (every, slice(0, p))), (1, (every,), 0, (every, slice(p, 2 * p)))],
    )[0]


def product_kernel(start, tile, kept, sent, own_ref, near_ref, weight_ref, kept_ref, sent_ref, held_ref, both_ref, terms_ref, sem):
    tokens, _ = own_ref.shape
    rows, width = kept_ref.shape[1:]
    first = lax.rem(lax.axis_index("dp"), 2) * (weight_ref.shape[0] // 2) + start
    copies = []
    for i in range(width // tile):
        at = pl.multiple_of(first + i * tile, LANES)
        copies.append(pltpu.make_async_copy(weight_ref.at[pl.ds(at, tile), :], held_ref.at[i], sem.at[i]))
    for copy in copies:
        copy.start()
    both_ref[:tokens, :] = own_ref[...]
    both_ref[tokens:, :] = near_ref[...]
    for i, copy in enumerate(copies):
        copy.wait()
        product = lax.dot_general(
            both_ref[...], held_ref[i], (((1,), (1,)), ((), ())), preferred_element_type=jnp.float32
        )
        if i:
            split_and_encode(terms_ref, kept, sent, kept_ref, sent_ref, (i - 1) * tile, tile)
        for t in range(terms_ref.shape[0]):
            terms_ref[t, :, i * tile : (i + 1) * tile] = product[t * rows : (t + 1) * rows, :]
    split_and_encode(terms_ref, kept, sent, kept_ref, sent_ref, width - tile, tile)


def products(own, near, weight, rows, start, width, tile, kept, sent):
    tokens, hidden = own.shape
    n = tokens // rows
    return pl.pallas_call(
        functools.partial(product_kernel, start, tile, kept, sent),
        out_shape=(
            pltpu.VMEM((n, rows, width), jnp.float32),
            pltpu.VMEM((n * rows + SUBLANES, width), jnp.bfloat16),
        ),
        in_specs=[*spaces(2), *spaces(1, pltpu.HBM)],
        out_specs=tuple(spaces(2)),
        scratch_shapes=[
            pltpu.VMEM((width // tile, tile, hidden), jnp.bfloat16),
            pltpu.VMEM((2 * tokens, hidden), jnp.bfloat16),
            pltpu.VMEM((2 * n, rows, width), jnp.float32),
            pltpu.SemaphoreType.DMA((width // tile,)),
        ],
        compiler_params=limit(14),
        cost_estimate=cost(4 * tokens * hidden * width, 2 * hidden * width),
        name="products",
    )(in_vmem(own), in_vmem(near), in_hbm(weight))


def halve_kernel(kept, sent, kept_ref, word_ref, next_ref, sent_ref, terms_ref):
    decode_and_add(kept_ref, word_ref, terms_ref)
    split_and_encode(terms_ref, kept, sent, next_ref, sent_ref)


def halve(held, word, kept, sent):
    n, rows, width = held.shape
    m = n // 2
    return pl.pallas_call(
        functools.partial(halve_kernel, kept, sent),
        out_shape=(
            pltpu.VMEM((m, rows, width), jnp.float32),
            pltpu.VMEM((m * rows + SUBLANES, width), jnp.bfloat16),
        ),
        in_specs=spaces(2),
        out_specs=spaces(2),
        scratch_shapes=[pltpu.VMEM((n, rows, width), jnp.float32)],
        compiler_params=limit(5),
        cost_estimate=cost(1e9, 1e6),
        name="halve",
    )(in_vmem(held), in_vmem(word))


def finish_kernel(kept_ref, word_ref, mine_ref, other_ref, terms_ref):
    decode_and_add(kept_ref, word_ref, terms_ref)
    mine_ref[...] = terms_ref[0].astype(jnp.bfloat16)
    other_ref[...] = terms_ref[1].astype(jnp.bfloat16)


def finish(held, word):
    n, rows, width = held.shape
    shape = pltpu.VMEM((rows, width), jnp.bfloat16)
    return pl.pallas_call(
        finish_kernel,
        out_shape=(shape, shape),
        in_specs=spaces(2),
        out_specs=spaces(2),
        scratch_shapes=[pltpu.VMEM((n, rows, width), jnp.float32)],
        compiler_params=limit(5),
        cost_estimate=cost(5e8, 1e6),
        name="finish",
    )(in_vmem(held), in_vmem(word))


def begin_kernel(tile, early_ref, grads_ref, sum_ref):
    for at in range(0, early_ref.shape[1], tile):
        turned = early_ref[:, at : at + tile].T
        sum_ref[at : at + tile, :] = jnp.dot(turned, grads_ref[...], preferred_element_type=jnp.float32)


def begin(early, grads, tile):
    width, hidden = early.shape[1], grads.shape[1]
    return pl.pallas_call(
        functools.partial(begin_kernel, tile),
        out_shape=pltpu.VMEM((width, hidden), jnp.float32),
        in_specs=spaces(2),
        out_specs=spaces(1)[0],
        compiler_params=limit(6),
        cost_estimate=cost(2 * early.shape[0] * width * hidden, 1e6),
        name="begin",
    )(in_vmem(early), in_vmem(grads))


def outer_kernel(start, tile, chunk, count, late_ref, grads_ref, begun_ref, *rest):
    piece_refs = rest[:count]
    turned_ref, ready_ref, sem = rest[-3:]
    out_ref = rest[-5] if count else rest[-4]
    copies = []
    if count:
        whole_ref = rest[-4]
        core = lax.rem(lax.axis_index("dp"), 2)
        half = whole_ref.shape[1] // 2
        at = 0
        for c, ref in enumerate(piece_refs):
            side = core if c < count // 2 else 1 - core
            at = 0 if c == count // 2 else at
            columns = pl.ds(pl.multiple_of(side * half + at, LANES), ref.shape[1])
            copies.append(pltpu.make_async_copy(ref, whole_ref.at[:, columns], sem.at[c]))
            copies[-1].start()
            at += ref.shape[1]
    for first in range(0, late_ref.shape[1], tile):
        turned_ref[...] = late_ref[:, first : first + tile].T
        for at in range(0, tile, chunk):
            here = slice(first + at, first + at + chunk)
            ready_ref[here, :] = begun_ref[here, :] + jnp.dot(
                turned_ref[at : at + chunk, :], grads_ref[...], preferred_element_type=jnp.float32
            )
            there = slice(start + first + at, start + first + at + chunk)
            copies.append(
                pltpu.make_async_copy(ready_ref.at[here, :], out_ref.at[there, :], sem.at[len(copies)])
            )
            copies[-1].start()
    for copy in copies:
        copy.wait()


def outer(late, grads, begun, total, start, tile, chunk, into, pieces):
    width = late.shape[1]
    tokens, hidden = grads.shape
    count = len(pieces)
    operands = [in_vmem(x) for x in (late, grads, begun, *pieces)]
    in_specs = spaces(len(operands))
    aliases = {}
    if into is not None:
        aliases = {len(operands): 0}
        operands.append(in_hbm(into))
        in_specs = in_specs + spaces(1, pltpu.HBM)
    out_shape = [jax.ShapeDtypeStruct((total, hidden), jnp.float32)]
    if count:
        columns = sum(x.shape[1] for x in pieces)
        out_shape.append(jax.ShapeDtypeStruct((pieces[0].shape[0], columns), jnp.bfloat16))
    return pl.pallas_call(
        functools.partial(outer_kernel, start, tile, chunk, count),
        out_shape=tuple(out_shape),
        in_specs=in_specs,
        out_specs=tuple(spaces(len(out_shape), pltpu.HBM)),
        scratch_shapes=[
            pltpu.VMEM((tile, tokens), jnp.bfloat16),
            pltpu.VMEM((width, hidden), jnp.float32),
            pltpu.SemaphoreType.DMA((count + width // chunk,)),
        ],
        input_output_aliases=aliases,
        compiler_params=limit(12),
        cost_estimate=cost(2 * tokens * width * hidden, 4 * width * hidden),
        name="outer",
    )(*operands)


def tile_of(width, most):
    for count in range(1, width // LANES + 1):
        if width % count == 0 and width // count % LANES == 0 and width // count <= most:
            return width // count
    return None


def split_lists(labels, bit):
    kept = [i for i, (_, r) in enumerate(labels) if not r & bit]
    sent = [labels.index((labels[i][0], labels[i][1] ^ bit)) for i in kept]
    return kept, sent


def tiled_plan(activations, grad_out, weight):
    replicas, ranks = lax.axis_size("dp"), lax.axis_size("tensor")
    chips = replicas // 2
    rows, features = activations.shape
    own_block = features // replicas
    steps = replica_steps(replicas)
    bits = bits_of(ranks)
    relative = relatives(ranks)
    every = slice(None)

    *blocks, own = prepare(activations, grad_out, replicas, ranks)
    near = from_replica(own, 0, 1)
    pieces = [blocks[0]]
    for k in range(1, len(steps)):
        pieces.append(from_replica(blocks[k], *steps[k]))

    row_tile = tile_of(own_block, own_block // 3)
    cuts = {"a": (0, own_block - row_tile), "b": (own_block - row_tile, row_tile)}
    (local,) = arrange(
        pieces,
        [(len(steps), 1, rows, own_block)],
        [(k, (every,), 0, (k, 0)) for k in range(len(steps))],
    )
    came = flip(local, "tensor", bits[-1])
    gathered = arrange(
        [local, came],
        [(len(steps), 2, rows, width) for _, width in cuts.values()],
        [
            (p, (every, 0, every, slice(start, start + width)), c, (every, p))
            for p in (0, 1)
            for c, (start, width) in enumerate(cuts.values())
        ],
    )

    grads = [own, near]
    for s in range(1, chips):
        grads.append(from_replica(own, s, 0))
        grads.append(from_replica(grads[-1], 0, 1))
    tokens, hidden = grad_out.shape
    part = tokens // 2
    early_grads, late_grads = arrange(
        grads,
        [(len(grads) * part, hidden)] * 2,
        [
            (k, (slice(o * part, (o + 1) * part),), o, (slice(k * part, (k + 1) * part),))
            for k in range(len(grads))
            for o in (0, 1)
        ],
    )

    half = features // 2
    chunks = {"a": (0, half // 2, SUM_A), "b": (half // 2, half // 2, SUM_B)}
    mine, other = [], []
    for (start, width, places) in chunks.values():
        labels = [(c, r) for c in (0, 1) for r in relative]
        for i, place in enumerate(places):
            b = bits[place]
            kept, sent = split_lists(labels, b)
            if i == 0:
                held, word = products(own, near, weight, rows, start, width, tile_of(width, 384), kept, sent)
            else:
                held, word = halve(held, word, kept, sent)
            labels = [labels[i] for i in kept]
            word = flip(word, "tensor", b)
        keep, give = finish(held, word)
        mine.append(keep)
        other.append(from_replica(give, 0, 1))
    weight_grad = None
    for held, (name, (start, width)) in zip(gathered, cuts.items()):
        for i, b in enumerate(bits[-2::-1], 1):
            came = flip(held, "tensor", b)
            if i < len(bits) - 1:
                held = joined(held, came)
        flat = (replicas * ranks // 2 * rows, width)
        begun = begin(held.reshape(flat), early_grads, row_tile)
        weight_grad, *rest = outer(
            came.reshape(flat),
            late_grads,
            begun,
            own_block,
            start,
            row_tile,
            row_tile // OUT_CHUNKS,
            weight_grad,
            mine + other if name == "b" else [],
        )
    return (rest[0], weight_grad)


def plain_halves(blocks, mine):
    kept = lax.dynamic_index_in_dim(blocks, mine, 1, keepdims=False)
    sent = lax.dynamic_index_in_dim(blocks, 1 - mine, 1, keepdims=False)
    return kept, sent


def plain_scatter(partial, axis):
    size = lax.axis_size(axis)
    me = lax.axis_index(axis)
    rows, cols = partial.shape
    running = partial.reshape(size, rows // size, cols)
    for bit in [1 << k for k in range(size.bit_length() - 1)]:
        pairs = running.reshape(running.shape[0] // 2, 2, rows // size, cols)
        kept, sent = plain_halves(pairs, (me // bit) % 2)
        running = kept + flip(sent, axis, bit)
    return running[0]


def plain_gather(block, axis):
    size = lax.axis_size(axis)
    me = lax.axis_index(axis)
    held = block[None]
    for bit in reversed([1 << k for k in range(size.bit_length() - 1)]):
        other = flip(held, axis, bit)
        mine = (me // bit) % 2
        low = jnp.where(mine == 0, held, other)
        high = jnp.where(mine == 0, other, held)
        held = jnp.stack([low, high], 1).reshape(2 * held.shape[0], *held.shape[1:])
    return held


def plain_plan(activations, grad_out, weight):
    ranks = lax.axis_size("tensor")
    chips = lax.axis_size("dp") // 2
    me = lax.axis_index("dp")
    chip, core = me // 2, me % 2
    shard_rows, features = activations.shape
    wide = features // chips

    def block_for(step):
        return lax.dynamic_slice_in_dim(activations, ((chip + step) % chips) * wide, wide, 1)

    rows = [block_for(0)] + [from_replica(block_for(k), k, 0) for k in range(1, chips)]
    grads_near = from_replica(grad_out, 0, 1)
    grads_far = [from_replica(grad_out, k, 0) for k in range(1, chips)]
    partial = lax.dot_general(
        grad_out, weight, (((1,), (1,)), ((), ())), preferred_element_type=jnp.float32
    )
    held = plain_gather(jnp.stack(rows), "tensor")
    held = held.transpose(1, 0, 2, 3).reshape(chips * ranks * shard_rows, 2, wide // 2)
    kept, sent = plain_halves(held, core)
    columns = jnp.concatenate([kept, from_replica(sent, 0, 1)])
    grads = jnp.concatenate(
        [grad_out, *grads_far, grads_near, *[from_replica(g, 0, 1) for g in grads_far]]
    )
    input_grad = plain_scatter(partial, "tensor").astype(jnp.bfloat16)
    weight_grad = lax.dot_general(
        columns, grads, (((0,), (0,)), ((), ())), preferred_element_type=jnp.float32
    )
    return (input_grad, weight_grad)


def on_device(activations, grad_out, weight):
    rows, features = activations.shape
    ranks = lax.axis_size("tensor")
    blocks = features // lax.axis_size("dp")
    fits = (
        rows % SUBLANES == 0
        and 4 <= ranks <= SUBLANES
        and blocks % (3 * LANES) == 0
        and grad_out.shape[1] % LANES == 0
    )
    plan = tiled_plan if fits else plain_plan
    return plan(activations, grad_out, weight)


def solution(mesh):
    placed = (P(("dp", "tensor"), None), P("dp", "tensor"), P(None, "tensor"))
    return jax.shard_map(
        on_device,
        mesh=mesh,
        in_specs=placed,
        out_specs=(P(("dp", "tensor"), None), P("dp", "tensor")),
        check_vma=False,
    )
```

```python
import functools

import jax
import jax.numpy as jnp
from jax import lax
from jax.experimental import pallas as pl
from jax.experimental.pallas import tpu as pltpu
from jax.sharding import PartitionSpec as P

LANES = 128
SUBLANES = 8
SUM_A = (0, 1, 2)
SUM_B = (0, 1, 2)
OUT_CHUNKS = 1
OUT_TILE = 128
FULL_TILE = 512
CUT_SHARE = 3
STEEP = 127.0
LOW = 2.0**-3.5
SMALLEST = 1e-30


def cost(flops, nbytes):
    return pl.CostEstimate(flops=int(flops), bytes_accessed=int(nbytes), transcendentals=0)


def flip(value, axis, bit):
    pairs = [(i, i ^ bit) for i in range(lax.axis_size(axis))]
    return lax.ppermute(value, axis, pairs)


def from_replica(value, step, swap):
    size = lax.axis_size("dp")
    pairs = [(i, ((i // 2 + step) % (size // 2)) * 2 + (i % 2 ^ swap)) for i in range(size)]
    return lax.ppermute(value, "dp", pairs)


def to_word(value, peak):
    t = LOW + jnp.abs(value) * ((STEEP * LOW) / peak)
    for _ in range(5):
        t = t * t
    return jnp.where(value < 0, -t, t)


def from_word(word, peak):
    t = jnp.exp2(jnp.log2(jnp.abs(word)) * (1.0 / 32.0))
    size = (t - LOW) * (peak * (1.0 / (STEEP * LOW)))
    return jnp.where(word < 0, -size, size)


def block_peak(value):
    top = jnp.maximum(jnp.max(jnp.abs(value)), SMALLEST)
    return top.astype(jnp.bfloat16).astype(jnp.float32)


def in_vmem(value):
    return pltpu.with_memory_space_constraint(value, pltpu.VMEM)


def in_hbm(value):
    return pltpu.with_memory_space_constraint(value, pltpu.HBM)


def spaces(count, where=pltpu.VMEM):
    return [pl.BlockSpec(memory_space=where)] * count


def limit(mebibytes):
    return pltpu.CompilerParams(vmem_limit_bytes=mebibytes * 1024 * 1024)


def split_and_encode(terms_ref, kept, sent, kept_ref, sent_ref, start=0, width=None):
    n, rows, cols = kept_ref.shape
    width = cols if width is None else width
    here = slice(start, start + width)
    for m in range(n):
        kept_ref[m, :, here] = terms_ref[kept[m], :, here]
        gone = terms_ref[sent[m], :, here]
        peak = block_peak(gone)
        sent_ref[m * rows : (m + 1) * rows, here] = to_word(gone, peak).astype(jnp.bfloat16)
        sent_ref[n * rows + m : n * rows + m + 1, here] = jnp.full((1, width), peak, jnp.bfloat16)
    if n < SUBLANES:
        sent_ref[n * rows + n :, here] = jnp.zeros((SUBLANES - n, width), jnp.bfloat16)


def decode_and_add(kept_ref, word_ref, terms_ref):
    n, rows, _ = kept_ref.shape
    peaks = word_ref[n * rows : n * rows + SUBLANES, :].astype(jnp.float32)
    for m in range(n):
        word = word_ref[m * rows : (m + 1) * rows, :].astype(jnp.float32)
        terms_ref[m] = kept_ref[m] + from_word(word, peaks[m : m + 1, :])


def relatives(ranks):
    found = [0]
    for b in reversed(bits_of(ranks)):
        found += [r ^ b for r in found]
    return found


def bits_of(size):
    return [1 << k for k in range(size.bit_length() - 1)]


def replica_steps(replicas):
    return [(s, w) for s in range(replicas // 2) for w in (0, 1)]


def prepare_kernel(acts_ref, grads_ref, *refs):
    piece_refs, turned_ref, sem = refs[:-2], refs[-2], refs[-1]
    rows, width = piece_refs[0].shape
    replicas = len(piece_refs)
    me, rank = lax.axis_index("dp"), lax.axis_index("tensor")
    copies = []
    for p, r in enumerate(relatives(turned_ref.shape[0] // rows)):
        start = pl.multiple_of(lax.bitwise_xor(rank, jnp.int32(r)) * rows, SUBLANES)
        copies.append(
            pltpu.make_async_copy(
                grads_ref.at[pl.ds(start, rows), :], turned_ref.at[p * rows : (p + 1) * rows, :], sem.at[p]
            )
        )
    for (s, w), ref in zip(replica_steps(replicas), piece_refs):
        chip = lax.rem(lax.div(me, 2) + s, replicas // 2)
        to = chip * 2 + lax.bitwise_xor(lax.rem(me, 2), jnp.int32(w))
        start = pl.multiple_of(to * width, LANES)
        copies.append(pltpu.make_async_copy(acts_ref.at[:, pl.ds(start, width)], ref, sem.at[len(copies)]))
    for copy in copies:
        copy.start()
    for copy in copies:
        copy.wait()


def prepare(activations, grads, replicas, ranks):
    rows, features = activations.shape
    width = features // replicas
    out_shape = [pltpu.VMEM((rows, width), jnp.bfloat16)] * replicas
    return pl.pallas_call(
        prepare_kernel,
        out_shape=(*out_shape, pltpu.VMEM(grads.shape, jnp.bfloat16)),
        in_specs=spaces(2, pltpu.HBM),
        out_specs=tuple(spaces(replicas + 1)),
        scratch_shapes=[pltpu.SemaphoreType.DMA((replicas + ranks,))],
        compiler_params=limit(4),
        cost_estimate=cost(1e8, 3e6),
        name="prepare",
    )(in_hbm(activations), in_hbm(grads))


def copy_kernel(plan, *refs):
    for source, source_at, target, target_at in plan:
        refs[target][target_at] = refs[source][source_at]


def arrange(arrays, shapes, plan):
    count = len(arrays)
    found = pl.pallas_call(
        functools.partial(copy_kernel, [(i, at, count + o, to) for i, at, o, to in plan]),
        out_shape=tuple(pltpu.VMEM(shape, jnp.bfloat16) for shape in shapes),
        in_specs=spaces(count),
        out_specs=tuple(spaces(len(shapes))),
        compiler_params=limit(4),
        cost_estimate=cost(1e8, 1e6),
        name="arrange",
    )(*[in_vmem(x) for x in arrays])
    return found


def joined(first, second):
    k, p, rows, width = first.shape
    every = slice(None)
    return arrange(
        [first, second],
        [(k, 2 * p, rows, width)],
        [(0, (every,), 0, (every, slice(0, p))), (1, (every,), 0, (every, slice(p, 2 * p)))],
    )[0]


def product_kernel(
    start, tiles, kept, sent, own_ref, near_ref, weight_ref, kept_ref, sent_ref, held_ref, both_ref, terms_ref, sem
):
    tokens, _ = own_ref.shape
    rows, _ = kept_ref.shape[1:]
    first = lax.rem(lax.axis_index("dp"), 2) * (weight_ref.shape[0] // 2) + start
    starts = [sum(tiles[:i]) for i in range(len(tiles))]
    copies = []
    for i, (begin_at, tile) in enumerate(zip(starts, tiles)):
        at = pl.multiple_of(first + begin_at, LANES)
        copies.append(
            pltpu.make_async_copy(
                weight_ref.at[pl.ds(at, tile), :], held_ref.at[begin_at : begin_at + tile, :], sem.at[i]
            )
        )
    for copy in copies:
        copy.start()
    both_ref[:tokens, :] = own_ref[...]
    both_ref[tokens:, :] = near_ref[...]
    last = None
    for copy, begin_at, tile in zip(copies, starts, tiles):
        copy.wait()
        product = lax.dot_general(
            both_ref[...],
            held_ref[begin_at : begin_at + tile, :],
            (((1,), (1,)), ((), ())),
            preferred_element_type=jnp.float32,
        )
        if last is not None:
            split_and_encode(terms_ref, kept, sent, kept_ref, sent_ref, *last)
        for t in range(terms_ref.shape[0]):
            terms_ref[t, :, begin_at : begin_at + tile] = product[t * rows : (t + 1) * rows, :]
        last = (begin_at, tile)
    split_and_encode(terms_ref, kept, sent, kept_ref, sent_ref, *last)


def products(own, near, weight, rows, start, width, tiles, kept, sent):
    tokens, hidden = own.shape
    n = tokens // rows
    return pl.pallas_call(
        functools.partial(product_kernel, start, tiles, kept, sent),
        out_shape=(
            pltpu.VMEM((n, rows, width), jnp.float32),
            pltpu.VMEM((n * rows + SUBLANES, width), jnp.bfloat16),
        ),
        in_specs=[*spaces(2), *spaces(1, pltpu.HBM)],
        out_specs=tuple(spaces(2)),
        scratch_shapes=[
            pltpu.VMEM((width, hidden), jnp.bfloat16),
            pltpu.VMEM((2 * tokens, hidden), jnp.bfloat16),
            pltpu.VMEM((2 * n, rows, width), jnp.float32),
            pltpu.SemaphoreType.DMA((len(tiles),)),
        ],
        compiler_params=limit(16),
        cost_estimate=cost(4 * tokens * hidden * width, 2 * hidden * width),
        name="products",
    )(in_vmem(own), in_vmem(near), in_hbm(weight))


def tiles_of(width):
    tiles = [FULL_TILE] * (width // FULL_TILE)
    return ([width % FULL_TILE] if width % FULL_TILE else []) + tiles


def halve_kernel(kept, sent, kept_ref, word_ref, next_ref, sent_ref, terms_ref):
    decode_and_add(kept_ref, word_ref, terms_ref)
    split_and_encode(terms_ref, kept, sent, next_ref, sent_ref)


def halve(held, word, kept, sent):
    n, rows, width = held.shape
    m = n // 2
    return pl.pallas_call(
        functools.partial(halve_kernel, kept, sent),
        out_shape=(
            pltpu.VMEM((m, rows, width), jnp.float32),
            pltpu.VMEM((m * rows + SUBLANES, width), jnp.bfloat16),
        ),
        in_specs=spaces(2),
        out_specs=spaces(2),
        scratch_shapes=[pltpu.VMEM((n, rows, width), jnp.float32)],
        compiler_params=limit(5),
        cost_estimate=cost(1e9, 1e6),
        name="halve",
    )(in_vmem(held), in_vmem(word))


def finish_kernel(kept_ref, word_ref, mine_ref, other_ref, terms_ref):
    decode_and_add(kept_ref, word_ref, terms_ref)
    mine_ref[...] = terms_ref[0].astype(jnp.bfloat16)
    other_ref[...] = terms_ref[1].astype(jnp.bfloat16)


def finish(held, word):
    n, rows, width = held.shape
    shape = pltpu.VMEM((rows, width), jnp.bfloat16)
    return pl.pallas_call(
        finish_kernel,
        out_shape=(shape, shape),
        in_specs=spaces(2),
        out_specs=spaces(2),
        scratch_shapes=[pltpu.VMEM((n, rows, width), jnp.float32)],
        compiler_params=limit(5),
        cost_estimate=cost(5e8, 1e6),
        name="finish",
    )(in_vmem(held), in_vmem(word))


def begin_kernel(tile, early_ref, grads_ref, sum_ref):
    for at in range(0, early_ref.shape[1], tile):
        turned = early_ref[:, at : at + tile].T
        sum_ref[at : at + tile, :] = jnp.dot(turned, grads_ref[...], preferred_element_type=jnp.float32)


def begin(early, grads, tile):
    width, hidden = early.shape[1], grads.shape[1]
    return pl.pallas_call(
        functools.partial(begin_kernel, tile),
        out_shape=pltpu.VMEM((width, hidden), jnp.float32),
        in_specs=spaces(2),
        out_specs=spaces(1)[0],
        compiler_params=limit(6),
        cost_estimate=cost(2 * early.shape[0] * width * hidden, 1e6),
        name="begin",
    )(in_vmem(early), in_vmem(grads))


def outer_kernel(start, tile, chunk, count, late_ref, grads_ref, begun_ref, *rest):
    piece_refs = rest[:count]
    turned_ref, ready_ref, sem = rest[-3:]
    out_ref = rest[-5] if count else rest[-4]
    copies = []
    if count:
        whole_ref = rest[-4]
        core = lax.rem(lax.axis_index("dp"), 2)
        half = whole_ref.shape[1] // 2
        at = 0
        for c, ref in enumerate(piece_refs):
            side = core if c < count // 2 else 1 - core
            at = 0 if c == count // 2 else at
            columns = pl.ds(pl.multiple_of(side * half + at, LANES), ref.shape[1])
            copies.append(pltpu.make_async_copy(ref, whole_ref.at[:, columns], sem.at[c]))
            copies[-1].start()
            at += ref.shape[1]
    for first in range(0, late_ref.shape[1], tile):
        turned_ref[...] = late_ref[:, first : first + tile].T
        for at in range(0, tile, chunk):
            here = slice(first + at, first + at + chunk)
            ready_ref[here, :] = begun_ref[here, :] + jnp.dot(
                turned_ref[at : at + chunk, :], grads_ref[...], preferred_element_type=jnp.float32
            )
            there = slice(start + first + at, start + first + at + chunk)
            copies.append(
                pltpu.make_async_copy(ready_ref.at[here, :], out_ref.at[there, :], sem.at[len(copies)])
            )
            copies[-1].start()
    for copy in copies:
        copy.wait()


def outer(late, grads, begun, total, start, tile, chunk, into, pieces):
    width = late.shape[1]
    tokens, hidden = grads.shape
    count = len(pieces)
    operands = [in_vmem(x) for x in (late, grads, begun, *pieces)]
    in_specs = spaces(len(operands))
    aliases = {}
    if into is not None:
        aliases = {len(operands): 0}
        operands.append(in_hbm(into))
        in_specs = in_specs + spaces(1, pltpu.HBM)
    out_shape = [jax.ShapeDtypeStruct((total, hidden), jnp.float32)]
    if count:
        columns = sum(x.shape[1] for x in pieces)
        out_shape.append(jax.ShapeDtypeStruct((pieces[0].shape[0], columns), jnp.bfloat16))
    return pl.pallas_call(
        functools.partial(outer_kernel, start, tile, chunk, count),
        out_shape=tuple(out_shape),
        in_specs=in_specs,
        out_specs=tuple(spaces(len(out_shape), pltpu.HBM)),
        scratch_shapes=[
            pltpu.VMEM((tile, tokens), jnp.bfloat16),
            pltpu.VMEM((width, hidden), jnp.float32),
            pltpu.SemaphoreType.DMA((count + width // chunk,)),
        ],
        input_output_aliases=aliases,
        compiler_params=limit(12),
        cost_estimate=cost(2 * tokens * width * hidden, 4 * width * hidden),
        name="outer",
    )(*operands)


def tile_of(width, most):
    for count in range(1, width // LANES + 1):
        if width % count == 0 and width // count % LANES == 0 and width // count <= most:
            return width // count
    return None


def split_lists(labels, bit):
    kept = [i for i, (_, r) in enumerate(labels) if not r & bit]
    sent = [labels.index((labels[i][0], labels[i][1] ^ bit)) for i in kept]
    return kept, sent


def tiled_plan(activations, grad_out, weight):
    replicas, ranks = lax.axis_size("dp"), lax.axis_size("tensor")
    chips = replicas // 2
    rows, features = activations.shape
    own_block = features // replicas
    steps = replica_steps(replicas)
    bits = bits_of(ranks)
    relative = relatives(ranks)
    every = slice(None)

    *blocks, own = prepare(activations, grad_out, replicas, ranks)
    near = from_replica(own, 0, 1)
    pieces = [blocks[0]]
    for k in range(1, len(steps)):
        pieces.append(from_replica(blocks[k], *steps[k]))

    last = max(1, own_block // LANES // CUT_SHARE) * LANES
    cuts = {"a": (0, own_block - last), "b": (own_block - last, last)}
    (local,) = arrange(
        pieces,
        [(len(steps), 1, rows, own_block)],
        [(k, (every,), 0, (k, 0)) for k in range(len(steps))],
    )
    came = flip(local, "tensor", bits[-1])
    gathered = arrange(
        [local, came],
        [(len(steps), 2, rows, width) for _, width in cuts.values()],
        [
            (p, (every, 0, every, slice(start, start + width)), c, (every, p))
            for p in (0, 1)
            for c, (start, width) in enumerate(cuts.values())
        ],
    )

    grads = [own, near]
    for s in range(1, chips):
        grads.append(from_replica(own, s, 0))
        grads.append(from_replica(grads[-1], 0, 1))
    tokens, hidden = grad_out.shape
    part = tokens // 2
    early_grads, late_grads = arrange(
        grads,
        [(len(grads) * part, hidden)] * 2,
        [
            (k, (slice(o * part, (o + 1) * part),), o, (slice(k * part, (k + 1) * part),))
            for k in range(len(grads))
            for o in (0, 1)
        ],
    )

    half = features // 2
    chunks = {"a": (0, half // 2, SUM_A), "b": (half // 2, half // 2, SUM_B)}
    mine, other = [], []
    for (start, width, places) in chunks.values():
        labels = [(c, r) for c in (0, 1) for r in relative]
        for i, place in enumerate(places):
            b = bits[place]
            kept, sent = split_lists(labels, b)
            if i == 0:
                held, word = products(own, near, weight, rows, start, width, tiles_of(width), kept, sent)
            else:
                held, word = halve(held, word, kept, sent)
            labels = [labels[i] for i in kept]
            word = flip(word, "tensor", b)
        keep, give = finish(held, word)
        mine.append(keep)
        other.append(from_replica(give, 0, 1))
    weight_grad = None
    for held, (name, (start, width)) in zip(gathered, cuts.items()):
        for i, b in enumerate(bits[-2::-1], 1):
            came = flip(held, "tensor", b)
            if i < len(bits) - 1:
                held = joined(held, came)
        flat = (replicas * ranks // 2 * rows, width)
        begun = begin(held.reshape(flat), early_grads, width)
        weight_grad, *rest = outer(
            came.reshape(flat),
            late_grads,
            begun,
            own_block,
            start,
            tile_of(width, OUT_TILE),
            tile_of(width, OUT_TILE) // OUT_CHUNKS,
            weight_grad,
            mine + other if name == "b" else [],
        )
    return (rest[0], weight_grad)


def plain_halves(blocks, mine):
    kept = lax.dynamic_index_in_dim(blocks, mine, 1, keepdims=False)
    sent = lax.dynamic_index_in_dim(blocks, 1 - mine, 1, keepdims=False)
    return kept, sent


def plain_scatter(partial, axis):
    size = lax.axis_size(axis)
    me = lax.axis_index(axis)
    rows, cols = partial.shape
    running = partial.reshape(size, rows // size, cols)
    for bit in [1 << k for k in range(size.bit_length() - 1)]:
        pairs = running.reshape(running.shape[0] // 2, 2, rows // size, cols)
        kept, sent = plain_halves(pairs, (me // bit) % 2)
        running = kept + flip(sent, axis, bit)
    return running[0]


def plain_gather(block, axis):
    size = lax.axis_size(axis)
    me = lax.axis_index(axis)
    held = block[None]
    for bit in reversed([1 << k for k in range(size.bit_length() - 1)]):
        other = flip(held, axis, bit)
        mine = (me // bit) % 2
        low = jnp.where(mine == 0, held, other)
        high = jnp.where(mine == 0, other, held)
        held = jnp.stack([low, high], 1).reshape(2 * held.shape[0], *held.shape[1:])
    return held


def plain_plan(activations, grad_out, weight):
    ranks = lax.axis_size("tensor")
    chips = lax.axis_size("dp") // 2
    me = lax.axis_index("dp")
    chip, core = me // 2, me % 2
    shard_rows, features = activations.shape
    wide = features // chips

    def block_for(step):
        return lax.dynamic_slice_in_dim(activations, ((chip + step) % chips) * wide, wide, 1)

    rows = [block_for(0)] + [from_replica(block_for(k), k, 0) for k in range(1, chips)]
    grads_near = from_replica(grad_out, 0, 1)
    grads_far = [from_replica(grad_out, k, 0) for k in range(1, chips)]
    partial = lax.dot_general(
        grad_out, weight, (((1,), (1,)), ((), ())), preferred_element_type=jnp.float32
    )
    held = plain_gather(jnp.stack(rows), "tensor")
    held = held.transpose(1, 0, 2, 3).reshape(chips * ranks * shard_rows, 2, wide // 2)
    kept, sent = plain_halves(held, core)
    columns = jnp.concatenate([kept, from_replica(sent, 0, 1)])
    grads = jnp.concatenate(
        [grad_out, *grads_far, grads_near, *[from_replica(g, 0, 1) for g in grads_far]]
    )
    input_grad = plain_scatter(partial, "tensor").astype(jnp.bfloat16)
    weight_grad = lax.dot_general(
        columns, grads, (((0,), (0,)), ((), ())), preferred_element_type=jnp.float32
    )
    return (input_grad, weight_grad)


def on_device(activations, grad_out, weight):
    rows, features = activations.shape
    ranks = lax.axis_size("tensor")
    blocks = features // lax.axis_size("dp")
    fits = (
        rows % SUBLANES == 0
        and 4 <= ranks <= SUBLANES
        and blocks % (3 * LANES) == 0
        and grad_out.shape[1] % LANES == 0
    )
    plan = tiled_plan if fits else plain_plan
    return plan(activations, grad_out, weight)


def solution(mesh):
    placed = (P(("dp", "tensor"), None), P("dp", "tensor"), P(None, "tensor"))
    return jax.shard_map(
        on_device,
        mesh=mesh,
        in_specs=placed,
        out_specs=(P(("dp", "tensor"), None), P("dp", "tensor")),
        check_vma=False,
    )
```
